64 devices in a mesh: rep: 8 (over x, y, core), dp: 8 (over z).
Axes of the slice: x: 2, y: 2, z: 8, core: 2. Of those that a mesh axis runs over, the one named last changes fastest.
The devices are a block of a 4x4x8 slice.
Arguments:
- x: bfloat16 [64, 2048, 768], P(('rep', 'dp')), parts along dimension 0
- dy: bfloat16 [64, 2048, 768], P(('rep', 'dp')), parts along dimension 0
- w_gate: bfloat16 [2, 768, 1792], replicated
- w_up: bfloat16 [2, 768, 1792], replicated
- w_down: bfloat16 [2, 1792, 768], replicated
- m_w_gate: float32 [2, 768, 1792], replicated
- m_w_up: float32 [2, 768, 1792], replicated
- m_w_down: float32 [2, 1792, 768], replicated
- v_w_gate: float32 [2, 768, 1792], replicated
- v_w_up: float32 [2, 768, 1792], replicated
- v_w_down: float32 [2, 1792, 768], replicated
Outputs:
- output 1: bfloat16 [16, 768, 1792], P('rep'), parts along dimension 0
- output 2: bfloat16 [16, 768, 1792], P('rep'), parts along dimension 0
- output 3: bfloat16 [16, 1792, 768], P('rep'), parts along dimension 0
- output 4: float32 [16, 768, 1792], P('rep'), parts along dimension 0
- output 5: float32 [16, 768, 1792], P('rep'), parts along dimension 0
- output 6: float32 [16, 1792, 768], P('rep'), parts along dimension 0
- output 7: float32 [16, 768, 1792], P('rep'), parts along dimension 0
- output 8: float32 [16, 768, 1792], P('rep'), parts along dimension 0
- output 9: float32 [16, 1792, 768], P('rep'), parts along dimension 0
There are 8 independent parts. The reference program is written for one: setup_inputs(seed, part) draws one part's arguments, and reference() takes and returns one part's arrays. A program takes and returns all parts, laid end to end along the dimension named above; an argument that names none is the same for every part.
All inputs are finite; a program needn't handle non-finite values.
Results may differ from the reference program's by a relative error of at most 0.022.
Values are sent between devices in bfloat16 or wider.
A program may use at most 768 MiB of HBM per device.

```python
import jax
import jax.numpy as jnp
from jax import lax

SEQUENCES = 8
TOKENS = 2048
D = 768
FF = 1792
LAYERS = 2
NAMES = ("w_gate", "w_up", "w_down")
SHAPES = {"w_gate": (LAYERS, D, FF), "w_up": (LAYERS, D, FF), "w_down": (LAYERS, FF, D)}


def bump(key, n, height):
    away = (jnp.arange(n, dtype=jnp.int32) - jax.random.randint(key, (), 0, n, jnp.int32)) % n
    return jnp.where(away < n // 8, height, 1.0)


def together(key, own, strength):
    shared = jax.random.normal(key, own.shape[1:], jnp.float32)
    return (own + strength * shared) * lax.rsqrt(1 + strength * strength)


def setup_inputs(seed: int = 0, part: int = 0) -> dict:
    kx, kdy, ka, kb, kz, kf, kh, kl, *keys = jax.random.split(jax.random.key(seed), 8 + 3 * len(NAMES))
    kx, kdy, ka, kb = (jax.random.fold_in(k, part) for k in (kx, kdy, ka, kb))
    kw, km, kv = (keys[i::3] for i in range(3))
    shape = (SEQUENCES, TOKENS, D)
    much_x, much_dy = jax.random.uniform(kz, (2,), jnp.float32, 0.0, 1.0)
    loud = 2.0 ** jax.random.uniform(jax.random.fold_in(kz, 1), (), jnp.float32, -1.0, 2.0)
    layers = 2.0 ** jax.random.uniform(kl, (LAYERS, 1, 1), jnp.float32, -1.0, 1.0)
    x = together(ka, jax.random.normal(kx, shape, jnp.float32), much_x) * bump(kf, D, 4.0)
    dy = together(kb, jax.random.normal(kdy, shape, jnp.float32), much_dy)
    drawn = {"x": x.astype(jnp.bfloat16), "dy": (loud * dy * (SEQUENCES * TOKENS) ** -0.5).astype(jnp.bfloat16)}
    for key, name in zip(kw, NAMES, strict=True):
        w = jax.random.normal(key, SHAPES[name], jnp.float32) * SHAPES[name][1] ** -0.5
        drawn[name] = (w * {"w_gate": 1.0, "w_up": bump(kh, FF, 4.0), "w_down": layers}[name]).astype(jnp.bfloat16)
    for key, name in zip(km, NAMES, strict=True):
        drawn[f"m_{name}"] = 0.1 * jax.random.normal(key, SHAPES[name], jnp.float32)
    for key, name in zip(kv, NAMES, strict=True):
        drawn[f"v_{name}"] = jax.random.uniform(key, SHAPES[name], jnp.float32, 0.005, 0.015)
    return drawn


def matmul(a, w):
    return jnp.dot(a, w, preferred_element_type=jnp.float32).astype(jnp.bfloat16)


def normed(h):
    wide = h.astype(jnp.float32)
    scale = lax.rsqrt(jnp.mean(wide**2, -1, keepdims=True) + 1e-6)
    return (wide * scale).astype(jnp.bfloat16)


def layer(h, w):
    a = normed(h)
    gate = jnp.dot(a, w["w_gate"], preferred_element_type=jnp.float32)
    up = jnp.dot(a, w["w_up"], preferred_element_type=jnp.float32)
    return h + matmul((jax.nn.silu(gate) * up).astype(jnp.bfloat16), w["w_down"])


def adamw(w, m, v, g):
    m = 0.9 * m + 0.1 * g
    v = 0.95 * v + 0.05 * g * g
    step = m * lax.rsqrt(v + 1e-8) + 0.1 * w
    return (w - 0.02 * step).astype(jnp.bfloat16), m, v


def clipped(gradients, sum_of_squares, count):
    factor = jnp.minimum(1.0, 0.5 * lax.rsqrt(sum_of_squares / count + 1e-30))
    return [g * factor for g in gradients]


def stack(weights, h):
    return lax.scan(lambda h, w: (layer(h, w), None), h, weights)[0]


def reference(x, dy, w_gate, w_up, w_down, m_w_gate, m_w_up, m_w_down, v_w_gate, v_w_up, v_w_down):
    weights = dict(zip(NAMES, (w_gate, w_up, w_down), strict=True))

    def take(so_far, sequence):
        h, by_y = sequence
        _, back = jax.vjp(lambda w: stack(w, h), weights)
        return jax.tree.map(lambda total, term: total + term.astype(jnp.float32), so_far, back(by_y)[0]), None

    none_yet = {name: jnp.zeros(w.shape, jnp.float32) for name, w in weights.items()}
    by_weights, _ = lax.scan(take, none_yet, (x, dy))
    gradients = [by_weights[name].astype(jnp.bfloat16).astype(jnp.float32) for name in NAMES]
    gradients = clipped(gradients, sum(jnp.sum(g * g) for g in gradients), sum(g.size for g in gradients))
    new = [
        adamw(w.astype(jnp.float32), m, v, g)
        for w, m, v, g in zip((w_gate, w_up, w_down), (m_w_gate, m_w_up, m_w_down), (v_w_gate, v_w_up, v_w_down), gradients, strict=True)
    ]
    return tuple(one[which] for which in range(3) for one in new)
```

```python
import functools

import jax
import jax.numpy as jnp
from jax import lax
from jax.experimental import pallas as pl
from jax.experimental.pallas import tpu as pltpu
from jax.sharding import PartitionSpec as P


BW = 256
RB = 3
f32, bf16 = jnp.float32, jnp.bfloat16
NT = (((1,), (1,)), ((), ()))
TN = (((0,), (0,)), ((), ()))

def mm(a, b, dims=(((1,), (0,)), ((), ()))):
    return lax.dot_general(a, b, dims, preferred_element_type=f32)

def rms_scale(wide):
    return lax.rsqrt(jnp.mean(wide * wide, -1, keepdims=True) + 1e-6)

def sigmoid(x):
    return 0.5 * jnp.tanh(0.5 * x) + 0.5

def kernel(cfg, x_in, dy_in, wg_in, wu_in, wd_in, own0, own1, ss, S, xh, a, aT, dh, hid, wg, wu, wd, recv,
           load_sem, x_sem, own_sem, send_sem, recv_sem, credit):
    n, T, D, F, tt, tb, comm = cfg["n"], cfg["T"], cfg["D"], cfg["F"], cfg["tt"], cfg["tb"], cfg["comm"]
    NB = F // BW
    NBLK = 2 * NB
    H = D // (2 * n)
    CH = 3 * H
    BR = 3 * D
    GB = NB * BR
    hr = BW // (2 * n)
    ncg = D // BW
    ramp = min(3, NBLK - 1)
    start = lambda b: jnp.where(b <= ramp, 2 * b, b + ramp)
    LAST = NBLK - 1 + ramp + n - 2
    me = lax.axis_index("dp")
    right, left = lax.rem(me + 1, n), lax.rem(me + n - 1, n)

    loads = [pltpu.make_async_copy(s, d, load_sem.at[i]) for i, (s, d) in enumerate((
        (x_in, xh), (wg_in.at[0], wg.at[0]), (wu_in.at[0], wu.at[0]), (wd_in.at[0], wd.at[0]), (dy_in, dh),
        (wg_in.at[1], wg.at[1]), (wu_in.at[1], wu.at[1]), (wd_in.at[1], wd.at[1])))]
    for c in loads[:4]:
        c.start()
    if comm:
        barrier = pltpu.get_barrier_semaphore()
        for nb in (left, right):
            pl.semaphore_signal(barrier, inc=1, device_id={"dp": nb}, device_id_type=pl.DeviceIdType.MESH)
    ss[...] = jnp.zeros_like(ss)

    def chunk_row(b, c, d):
        return pl.multiple_of(b * BR + (2 * c + d) * CH, 16)

    def chunk_of(s, d):
        return lax.rem(me + 2 * n - 1 - s, n) if d == 0 else lax.rem(me + 1 + s, n)

    def block_of(r, s):
        z = r - s
        b = jnp.where(z < 2 * ramp, lax.div(z, 2), z - ramp)
        return b, (z >= 0) & ((z >= 2 * ramp) | (lax.rem(z, 2) == 0)) & (b < NBLK)

    def hop(r, s, d):
        b, _ = block_of(r, s)
        slot = lax.rem(r, RB) * (n - 1) + s
        return pltpu.make_async_remote_copy(
            src_ref=S.at[pl.ds(chunk_row(b, chunk_of(s, d), d), CH), :], dst_ref=recv.at[d, slot],
            send_sem=send_sem.at[d, slot], recv_sem=recv_sem.at[d, slot],
            device_id={"dp": right if d == 0 else left}, device_id_type=pl.DeviceIdType.MESH)

    def arrival(d, slot):
        return pltpu.make_async_remote_copy(
            src_ref=recv.at[d, slot], dst_ref=recv.at[d, slot], send_sem=send_sem.at[d, slot], recv_sem=recv_sem.at[d, slot],
            device_id={"dp": right if d == 0 else left}, device_id_type=pl.DeviceIdType.MESH)

    def op(q, _):
        r, s = lax.div(q, n), lax.rem(q, n)
        b, live = block_of(r, s)
        @pl.when((s == 0) & (r >= RB) & (r <= LAST))
        def _():
            pl.semaphore_wait(credit.at[0], 1)
            pl.semaphore_wait(credit.at[1], 1)
        @pl.when(live & (s >= 1))
        def _():
            slot = lax.rem(r + RB - 1, RB) * (n - 1) + s - 1
            for d in range(2):
                arrival(d, slot).wait_recv()
                rows = pl.ds(chunk_row(b, chunk_of(s, d), d), CH)
                total = (S[rows, :].astype(f32) + recv[d, slot].astype(f32)).astype(bf16)
                S[rows, :] = total
                @pl.when(s == n - 1)
                def _():
                    t = total.astype(f32)
                    t = t * t
                    ss[...] += functools.reduce(jnp.add, [t[i * 8:(i + 1) * 8, h * 128:(h + 1) * 128] for i in range(CH // 8) for h in range(BW // 128)])
        @pl.when(live & (s == n - 1))
        def _():
            for d in range(2):
                pltpu.make_async_copy(S.at[pl.ds(chunk_row(b, me, d), CH), :], (own0, own1)[d].at[b], own_sem.at[d, b]).start()
        _, before = block_of(r - RB, s)
        @pl.when((s <= n - 2) & (r >= RB) & before)
        def _():
            for d in range(2):
                hop(r - RB, s, d).wait_send()
        @pl.when(live & (s <= n - 2))
        def _():
            for d in range(2):
                hop(r, s, d).start()
        @pl.when((s == n - 1) & (r >= 1) & (r <= LAST - RB + 1))
        def _():
            pl.semaphore_signal(credit.at[0], inc=1, device_id={"dp": left}, device_id_type=pl.DeviceIdType.MESH)
            pl.semaphore_signal(credit.at[1], inc=1, device_id={"dp": right}, device_id_type=pl.DeviceIdType.MESH)
        return 0

    def ops(q, count, ready):
        if not comm:
            return q
        limit = n * start(ready)
        end = jnp.where(q + count < limit, q + count, limit)
        lax.fori_loop(q, end, op, 0)
        return end

    for c in loads[:4]:
        c.wait()
    for c in loads[4:]:
        c.start()
    def fwd(t, _):
        rows = pl.ds(pl.multiple_of(t * tt, tt), tt)
        xw = xh[rows, :].astype(f32)
        at = (xw * rms_scale(xw)).astype(bf16)
        parts = []
        for j in range(NB):
            cols = slice(j * BW, (j + 1) * BW)
            g = mm(at, wg[0, :, cols])
            u = mm(at, wu[0, :, cols])
            parts.append((g * sigmoid(g) * u).astype(bf16))
        down = mm(jnp.concatenate(parts, axis=1), wd[0]).astype(bf16)
        h = (xw + down.astype(f32)).astype(bf16)
        xh[rows, :] = h
        hw = h.astype(f32)
        a1 = (hw * rms_scale(hw)).astype(bf16)
        a[rows, :] = a1
        aT[:, rows] = a1.T
        return 0
    lax.fori_loop(0, T // tt, fwd, 0)

    def block(l, j, dg0, du0, b, q, pace):
        cols = pl.ds(pl.multiple_of(j * BW, BW), BW)
        def tokens(t, q):
            q = ops(q, pace[0], b)
            rows = pl.ds(pl.multiple_of(t * tb, tb), tb)
            at = a[rows, :]
            g = mm(at, wg[l, :, cols])
            u = mm(at, wu[l, :, cols])
            dhid = mm(dh[rows, :], wd[l, cols, :], NT).astype(bf16).astype(f32)
            sg = sigmoid(g)
            s = g * sg
            hid[rows, :] = (s * u).astype(bf16)
            S[pl.ds(pl.multiple_of(du0 + t * tb, 16), tb), :] = (dhid * s).astype(bf16)
            S[pl.ds(pl.multiple_of(dg0 + t * tb, 16), tb), :] = (dhid * u * (sg + s * (1.0 - sg))).astype(bf16)
            return q
        q = lax.fori_loop(0, T // tb, tokens, q)
        base = b * BR
        def matmul_gate_up(k, row0):
            w = mm(aT[...], S[pl.ds(pl.multiple_of(row0, 16), T), :]).astype(bf16)
            for e in range(2 * n):
                S[pl.ds(pl.multiple_of(base + e * CH + k * H, 16), H), :] = w[e * H:(e + 1) * H]
        q = ops(q, pace[1], b)
        matmul_gate_up(0, dg0)
        q = ops(q, pace[1], b)
        matmul_gate_up(1, du0)
        q = ops(q, pace[1], b)
        w = mm(hid[...], dh[...], TN).astype(bf16)
        for e in range(2 * n):
            for cg in range(ncg):
                S[pl.ds(pl.multiple_of(base + e * CH + 2 * H + cg * hr, 16), hr), :] = w[e * hr:(e + 1) * hr, cg * BW:(cg + 1) * BW]
        return q

    for c in loads[4:]:
        c.wait()
    def last_layer(j, q):
        pace = jnp.where(j <= 2, n, 2)
        return block(1, j, GB + j * 2 * T, GB + j * 2 * T + T, j, q, (pace, pace))
    if comm:
        pl.semaphore_wait(barrier, 2)
    q = lax.fori_loop(0, NB, last_layer, 0)

    def d_input(t, q):
        q = ops(q, 3, NB)
        rows = pl.ds(pl.multiple_of(t * tt, tt), tt)
        dg = jnp.concatenate([S[pl.ds(pl.multiple_of(GB + j * 2 * T + t * tt, 16), tt), :] for j in range(NB)], axis=1)
        du = jnp.concatenate([S[pl.ds(pl.multiple_of(GB + j * 2 * T + T + t * tt, 16), tt), :] for j in range(NB)], axis=1)
        da = (mm(dg, wg[1], NT).astype(bf16).astype(f32) + mm(du, wu[1], NT).astype(bf16).astype(f32)).astype(bf16).astype(f32)
        wide = xh[rows, :].astype(f32)
        scale = rms_scale(wide)
        dot = jnp.sum(da * wide, -1, keepdims=True)
        dw = da * scale - wide * (scale * scale * scale * dot * (1.0 / D))
        dh[rows, :] = (dh[rows, :].astype(f32) + dw.astype(bf16).astype(f32)).astype(bf16)
        pltpu.make_async_copy(x_in.at[rows, :], xh.at[rows, :], x_sem).start()
        return q
    q = lax.fori_loop(0, T // tt, d_input, q)
    def renorm(t, q):
        rows = pl.ds(pl.multiple_of(t * tt, tt), tt)
        wide = xh[rows, :].astype(f32)
        a0 = (wide * rms_scale(wide)).astype(bf16)
        a[rows, :] = a0
        aT[:, rows] = a0.T
        return q
    pltpu.make_async_copy(x_in, xh, x_sem).wait()
    q = ops(q, 2, NB)
    lax.fori_loop(0, T // tt, renorm, 0)

    def first_layer(j, q):
        return block(0, j, 2 * GB, 2 * GB + T, NB + j, q, (1, 2))
    q = lax.fori_loop(0, NB, first_layer, q)
    if comm:
        lax.fori_loop(q, (LAST + 2) * n, op, 0)
        for r in range(LAST - RB + 2, LAST + 1):
            for s in range(n - 1):
                z = r - s
                b = z // 2 if z < 2 * ramp else z - ramp
                if z >= 0 and (z >= 2 * ramp or z % 2 == 0) and b < NBLK:
                    for d in range(2):
                        hop(r, s, d).wait_send()
        for d in range(2):
            for b in range(NBLK):
                pltpu.make_async_copy(S.at[pl.ds(0, CH), :], (own0, own1)[d].at[b], own_sem.at[d, b]).wait()
    else:
        cps = [pltpu.make_async_copy(S.at[pl.ds(b * BR + d * CH, CH), :], (own0, own1)[d].at[b], own_sem.at[d, b]) for d in range(2) for b in range(NBLK)]
        for c in cps: c.start()
        for c in cps: c.wait()

def k1(x, dy, wg, wu, wd, n, tt=256, tb=512, comm=True, cid=0):
    T, D = x.shape
    F = wg.shape[2]
    NB = F // BW
    NBLK = 2 * NB
    H = D // (2 * n); CH = 3 * H
    GB = NB * 3 * D
    cfg = dict(n=n, T=T, D=D, F=F, tt=min(tt, T), tb=min(tb, T), comm=comm)
    any_ = pl.BlockSpec(memory_space=pl.ANY)
    flops = 18 * 2 * T * D * F
    return pl.pallas_call(
        functools.partial(kernel, cfg),
        out_shape=(jax.ShapeDtypeStruct((NBLK, CH, BW), bf16),) * 2 + (jax.ShapeDtypeStruct((8, 128), f32),),
        in_specs=[any_] * 5,
        out_specs=(any_, any_, pl.BlockSpec(memory_space=pltpu.VMEM)),
        scratch_shapes=[
            pltpu.VMEM((max(GB + NB * 2 * T, 2 * GB + 2 * T), BW), bf16),
            pltpu.VMEM((T, D), bf16), pltpu.VMEM((T, D), bf16), pltpu.VMEM((D, T), bf16), pltpu.VMEM((T, D), bf16),
            pltpu.VMEM((T, BW), bf16),
            pltpu.VMEM((2, D, F), bf16), pltpu.VMEM((2, D, F), bf16), pltpu.VMEM((2, F, D), bf16),
            pltpu.VMEM((2, RB * (n - 1), CH, BW), bf16),
            pltpu.SemaphoreType.DMA((8,)), pltpu.SemaphoreType.DMA, pltpu.SemaphoreType.DMA((2, NBLK)),
            pltpu.SemaphoreType.DMA((2, RB * (n - 1))), pltpu.SemaphoreType.DMA((2, RB * (n - 1))), pltpu.SemaphoreType.REGULAR((2,)),
        ],
        compiler_params=pltpu.CompilerParams(vmem_limit_bytes=67043328, collective_id=cid if comm else None, has_side_effects=True),
        cost_estimate=pl.CostEstimate(flops=flops, bytes_accessed=40 * 10**6, transcendentals=0),
        name="grads")(x, dy, wg, wu, wd)


def adam_math(w, m, v, g):
    m = 0.9 * m + 0.1 * g
    v = 0.95 * v + 0.05 * g * g
    step = m * lax.rsqrt(v + 1e-8) + 0.1 * w
    return (w - 0.02 * step).astype(jnp.bfloat16), m, v

def opt_body(nb, idx_ref, fac_ref, p0, p1, wg, wu, wd, mg, mu, md, vg, vu, vd, *rest):
    outs = rest[-9:]
    factor = fac_ref[0]
    def one(p):
        for k,(w,m,v,o) in enumerate(((wg,mg,vg,0),(wu,mu,vu,1))):
            for j in range(nb):
                c = slice(j*BW,(j+1)*BW)
                g = p[0,j,k].astype(jnp.float32)*factor
                a,b,cc = adam_math(w[0,0,:,c].astype(jnp.float32), m[0,0,:,c], v[0,0,:,c], g)
                outs[o][0,0,:,c]=a; outs[3+o][0,0,:,c]=b; outs[6+o][0,0,:,c]=cc
        r = wd.shape[3]
        for j in range(nb):
            for q in range(wd.shape[4]//BW):
                c = slice(q*BW,(q+1)*BW)
                g = p[0,j,2,q*r:(q+1)*r].astype(jnp.float32)*factor
                a,b,cc = adam_math(wd[0,j,0,:,c].astype(jnp.float32), md[0,j,0,:,c], vd[0,j,0,:,c], g)
                outs[2][0,j,0,:,c]=a; outs[5][0,j,0,:,c]=b; outs[8][0,j,0,:,c]=cc
    d = pl.program_id(0)
    @pl.when(d==0)
    def _(): one(p0)
    @pl.when(d==1)
    def _(): one(p1)

def opt_call(idx, fac, p0, p1, ins, prev):
    L, nb = p0.shape[0], p0.shape[1]
    wg, wd = ins[0], ins[2]
    def gm(d,l,idx): return (l, jnp.where(d==0, idx[0], idx[1]), 0, 0)
    def dm(d,l,idx): return (l, 0, jnp.where(d==0, idx[0], idx[1]), 0, 0)
    gs = pl.BlockSpec((1,1)+wg.shape[2:], gm)
    ds = pl.BlockSpec((1,nb,1)+wd.shape[3:], dm)
    ps0 = pl.BlockSpec((1,)+p0.shape[1:], lambda d,l,idx:(L-1-jnp.where(d==0,l,L-1),0,0,0,0))
    ps1 = pl.BlockSpec((1,)+p0.shape[1:], lambda d,l,idx:(L-1-jnp.where(d==0,0,l),0,0,0,0))
    specs=[gs,gs,ds]*3
    any_=[pl.BlockSpec(memory_space=pl.ANY)]*9 if prev is not None else []
    fresh = prev is None
    grid_spec=pltpu.PrefetchScalarGridSpec(num_scalar_prefetch=1, grid=(2,L),
        in_specs=[pl.BlockSpec(memory_space=pltpu.SMEM),ps0,ps1]+specs+any_, out_specs=specs)
    odt=[jnp.bfloat16]*3+[jnp.float32]*6
    n=sum(x.size for x in ins[:3])
    return pl.pallas_call(functools.partial(opt_body,nb), grid_spec=grid_spec,
        out_shape=[jax.ShapeDtypeStruct(x.shape,t) for x,t in zip(ins,odt)],
        input_output_aliases={} if fresh else {13+i:i for i in range(9)},
        compiler_params=pltpu.CompilerParams(vmem_limit_bytes=62*2**20, dimension_semantics=("arbitrary","arbitrary")),
        cost_estimate=pl.CostEstimate(flops=int(5e9),bytes_accessed=22*10**6,transcendentals=0),
        name="adamw")(idx, fac, p0, p1, *ins, *(prev or []))
def views(arrs, n):
    out=[]
    for i,a in enumerate(arrs):
        L,r,c=a.shape
        if i%3<2: out.append(a.reshape(L,2*n,r//(2*n),c))
        else:
            nb=r//BW
            out.append(a.reshape(L,nb,2*n,BW//(2*n),c))
    return out


def solution(mesh):
    n = mesh.shape["dp"]
    right = [(i, (i + 1) % n) for i in range(n)]
    left = [(i, (i - 1) % n) for i in range(n)]

    def step(x, dy, *arrays):
        me = lax.axis_index("dp")
        own0, own1, squares = k1(x[0], dy[0], *arrays[:3], n)
        L, _, F = arrays[0].shape
        NB = F // BW
        ins = views(arrays, n)
        count = sum(w.size for w in arrays[:3])
        a, b = (o.reshape(L, NB, 3, o.shape[1] // 3, BW) for o in (own0, own1))
        factor, outs = None, None
        for s in range(n):
            na = nb = None
            if s < n - 1:
                na = lax.ppermute(a, "dp", right)
                nb = lax.ppermute(b, "dp", left)
            if factor is None:
                total = lax.psum(jnp.sum(squares), "dp")
                factor = jnp.minimum(1.0, 0.5 * lax.rsqrt(total / count + 1e-30)).reshape(1)
            c0, c1 = lax.rem(me - s + n, n), lax.rem(me + s, n)
            idx = jnp.stack([2 * c0, 2 * c1 + 1]).astype(jnp.int32)
            outs = opt_call(idx, factor, a, b, ins, outs)
            a, b = na, nb
        return tuple(o.reshape(w.shape) for o, w in zip(outs, arrays))

    step = jax.shard_map(
        step,
        mesh=mesh,
        in_specs=(P(("rep", "dp"), None, None),) * 2 + (P(None, None, None),) * 9,
        out_specs=(P("rep", None, None),) * 9,
        check_vma=False,
    )
    return step
```

```python
import functools

import jax
import jax.numpy as jnp
from jax import lax
from jax.experimental import pallas as pl
from jax.experimental.pallas import tpu as pltpu
from jax.sharding import PartitionSpec as P


BW = 256
RB = 3
f32, bf16 = jnp.float32, jnp.bfloat16
NT = (((1,), (1,)), ((), ()))
TN = (((0,), (0,)), ((), ()))


def mm(a, b, dims=(((1,), (0,)), ((), ()))):
    return lax.dot_general(a, b, dims, preferred_element_type=f32)


def rms_scale(wide):
    return lax.rsqrt(jnp.mean(wide * wide, -1, keepdims=True) + 1e-6)


def sigmoid(x):
    return 0.5 * jnp.tanh(0.5 * x) + 0.5


def kernel(cfg, x_in, dy_in, wg_in, wu_in, wd_in, own00, own01, own10, own11, ss, S, xh, a, aT, dh, hid, wg, wu, wd, recv,
           load_sem, x_sem, own_sem, send_sem, recv_sem, credit):
    n, T, D, F, tt, tb, comm = cfg["n"], cfg["T"], cfg["D"], cfg["F"], cfg["tt"], cfg["tb"], cfg["comm"]
    NB = F // BW
    NBLK = 2 * NB
    H = D // (2 * n)
    CH = 3 * H
    BR = 3 * D
    GB = NB * BR
    hr = BW // (2 * n)
    ncg = D // BW
    ramp = max(NBLK - 4, 1)
    start = lambda b: jnp.where(b <= ramp, 2 * b, b + ramp)
    LAST = NBLK - 1 + ramp + n - 2
    me = lax.axis_index("dp")
    right, left = lax.rem(me + 1, n), lax.rem(me + n - 1, n)

    loads = [pltpu.make_async_copy(s, d, load_sem.at[i]) for i, (s, d) in enumerate((
        (x_in, xh), (wg_in.at[0], wg.at[0]), (wu_in.at[0], wu.at[0]), (wd_in.at[0], wd.at[0]), (dy_in, dh),
        (wg_in.at[1], wg.at[1]), (wu_in.at[1], wu.at[1]), (wd_in.at[1], wd.at[1])))]
    for c in loads[:3]:
        c.start()
    if comm:
        barrier = pltpu.get_barrier_semaphore()
        for nb in (left, right):
            pl.semaphore_signal(barrier, inc=1, device_id={"dp": nb}, device_id_type=pl.DeviceIdType.MESH)
    ss[...] = jnp.zeros_like(ss)

    def chunk_row(b, c, d):
        return pl.multiple_of(b * BR + (2 * c + d) * CH, 16)

    def chunk_of(s, d):
        return lax.rem(me + 2 * n - 1 - s, n) if d == 0 else lax.rem(me + 1 + s, n)

    def block_of(r, s):
        z = r - s
        b = jnp.where(z < 2 * ramp, lax.div(z, 2), z - ramp)
        return b, (z >= 0) & ((z >= 2 * ramp) | (lax.rem(z, 2) == 0)) & (b < NBLK)

    def hop(r, s, d):
        b, _ = block_of(r, s)
        slot = lax.rem(r, RB) * (n - 1) + s
        return pltpu.make_async_remote_copy(
            src_ref=S.at[pl.ds(chunk_row(b, chunk_of(s, d), d), CH), :], dst_ref=recv.at[d, slot],
            send_sem=send_sem.at[d, slot], recv_sem=recv_sem.at[d, slot],
            device_id={"dp": right if d == 0 else left}, device_id_type=pl.DeviceIdType.MESH)

    def arrival(d, slot):
        return pltpu.make_async_remote_copy(
            src_ref=recv.at[d, slot], dst_ref=recv.at[d, slot], send_sem=send_sem.at[d, slot], recv_sem=recv_sem.at[d, slot],
            device_id={"dp": right if d == 0 else left}, device_id_type=pl.DeviceIdType.MESH)

    def op(q, _):
        r, s = lax.div(q, n), lax.rem(q, n)
        b, live = block_of(r, s)
        @pl.when((s == 0) & (r >= RB) & (r <= LAST))
        def _():
            pl.semaphore_wait(credit.at[0], 1)
            pl.semaphore_wait(credit.at[1], 1)
        @pl.when(live & (s >= 1))
        def _():
            slot = lax.rem(r + RB - 1, RB) * (n - 1) + s - 1
            for d in range(2):
                arrival(d, slot).wait_recv()
                rows = pl.ds(chunk_row(b, chunk_of(s, d), d), CH)
                total = (S[rows, :].astype(f32) + recv[d, slot].astype(f32)).astype(bf16)
                S[rows, :] = total
                @pl.when(s == n - 1)
                def _():
                    t = total.astype(f32)
                    t = t * t
                    ss[...] += functools.reduce(jnp.add, [t[i * 8:(i + 1) * 8, h * 128:(h + 1) * 128] for i in range(CH // 8) for h in range(BW // 128)])
        @pl.when(live & (s == n - 1))
        def _():
            for d in range(2):
                rows = pl.ds(chunk_row(b, me, d), CH)
                @pl.when(b < NB)
                def _():
                    pltpu.make_async_copy(S.at[rows, :], (own00, own01)[d].at[b], own_sem.at[d, b]).start()
                @pl.when(b >= NB)
                def _():
                    pltpu.make_async_copy(S.at[rows, :], (own10, own11)[d].at[b - NB], own_sem.at[d, b]).start()
        _, before = block_of(r - RB, s)
        @pl.when((s <= n - 2) & (r >= RB) & before)
        def _():
            for d in range(2):
                hop(r - RB, s, d).wait_send()
        @pl.when(live & (s <= n - 2))
        def _():
            for d in range(2):
                hop(r, s, d).start()
        @pl.when((s == n - 1) & (r >= 1) & (r <= LAST - RB + 1))
        def _():
            pl.semaphore_signal(credit.at[0], inc=1, device_id={"dp": left}, device_id_type=pl.DeviceIdType.MESH)
            pl.semaphore_signal(credit.at[1], inc=1, device_id={"dp": right}, device_id_type=pl.DeviceIdType.MESH)
        return 0

    def ops(q, count, ready):
        if not comm:
            return q
        limit = n * start(ready)
        end = jnp.where(q + count < limit, q + count, limit)
        lax.fori_loop(q, end, op, 0)
        return end

    loads[0].wait()
    loads[3].start()
    loads[1].wait()
    loads[2].wait()
    def fwd(t, _):
        rows = pl.ds(pl.multiple_of(t * tt, tt), tt)
        xw = xh[rows, :].astype(f32)
        at = (xw * rms_scale(xw)).astype(bf16)
        for j in range(NB):
            cols = slice(j * BW, (j + 1) * BW)
            g = mm(at, wg[0, :, cols])
            u = mm(at, wu[0, :, cols])
            S[pl.ds(pl.multiple_of(GB + j * T + t * tt, 16), tt), :] = (g * sigmoid(g) * u).astype(bf16)
        return 0
    lax.fori_loop(0, T // tt, fwd, 0)
    loads[3].wait()
    for c in loads[4:]:
        c.start()
    def fwd_down(t, _):
        rows = pl.ds(pl.multiple_of(t * tt, tt), tt)
        hidden = jnp.concatenate([S[pl.ds(pl.multiple_of(GB + j * T + t * tt, 16), tt), :] for j in range(NB)], axis=1)
        h = (xh[rows, :].astype(f32) + mm(hidden, wd[0]).astype(bf16).astype(f32)).astype(bf16)
        xh[rows, :] = h
        hw = h.astype(f32)
        a1 = (hw * rms_scale(hw)).astype(bf16)
        a[rows, :] = a1
        aT[:, rows] = a1.T
        return 0
    lax.fori_loop(0, T // tt, fwd_down, 0)

    def block(l, j, dg0, du0, b, q, pace):
        cols = pl.ds(pl.multiple_of(j * BW, BW), BW)
        q = ops(q, pace, b)
        def tokens(t, q):
            rows = pl.ds(pl.multiple_of(t * tb, tb), tb)
            at = a[rows, :]
            g = mm(at, wg[l, :, cols])
            u = mm(at, wu[l, :, cols])
            dhid = mm(dh[rows, :], wd[l, cols, :], NT).astype(bf16).astype(f32)
            sg = sigmoid(g)
            s = g * sg
            hid[rows, :] = (s * u).astype(bf16)
            S[pl.ds(pl.multiple_of(du0 + t * tb, 16), tb), :] = (dhid * s).astype(bf16)
            S[pl.ds(pl.multiple_of(dg0 + t * tb, 16), tb), :] = (dhid * u * (sg + s * (1.0 - sg))).astype(bf16)
            return q
        q = lax.fori_loop(0, T // tb, tokens, q, unroll=True)
        base = b * BR
        def gate_up(w, k):
            for e in range(2 * n):
                S[pl.ds(pl.multiple_of(base + e * CH + k * H, 16), H), :] = w[e * H:(e + 1) * H]
        def down(w):
            for e in range(2 * n):
                for cg in range(ncg):
                    S[pl.ds(pl.multiple_of(base + e * CH + 2 * H + cg * hr, 16), hr), :] = w[e * hr:(e + 1) * hr, cg * BW:(cg + 1) * BW]
        dgv = lambda: S[pl.ds(pl.multiple_of(dg0, 16), T), :]
        duv = lambda: S[pl.ds(pl.multiple_of(du0, 16), T), :]
        q = ops(q, pace, b)
        w = mm(aT[...], jnp.concatenate([dgv(), duv()], axis=1)).astype(bf16)
        gate_up(w[:, :BW], 0)
        gate_up(w[:, BW:], 1)
        down(mm(hid[...], dh[...], TN).astype(bf16))
        return q

    for c in loads[4:]:
        c.wait()
    def last_layer(j, q):
        return block(1, j, GB + j * 2 * T, GB + j * 2 * T + T, j, q, jnp.where(j <= 2, n, cfg["pace"][0]))
    if comm:
        pl.semaphore_wait(barrier, 2)
    q = lax.fori_loop(0, NB, last_layer, 0)

    def d_input(t, q):
        q = ops(q, cfg["pace"][1], NB)
        rows = pl.ds(pl.multiple_of(t * tt, tt), tt)
        dg = jnp.concatenate([S[pl.ds(pl.multiple_of(GB + j * 2 * T + t * tt, 16), tt), :] for j in range(NB)], axis=1)
        du = jnp.concatenate([S[pl.ds(pl.multiple_of(GB + j * 2 * T + T + t * tt, 16), tt), :] for j in range(NB)], axis=1)
        da = (mm(dg, wg[1], NT).astype(bf16).astype(f32) + mm(du, wu[1], NT).astype(bf16).astype(f32)).astype(bf16).astype(f32)
        wide = xh[rows, :].astype(f32)
        scale = rms_scale(wide)
        dot = jnp.sum(da * wide, -1, keepdims=True)
        dw = da * scale - wide * (scale * scale * scale * dot * (1.0 / D))
        dh[rows, :] = (dh[rows, :].astype(f32) + dw.astype(bf16).astype(f32)).astype(bf16)
        pltpu.make_async_copy(x_in.at[rows, :], xh.at[rows, :], x_sem).start()
        return q
    q = lax.fori_loop(0, T // tt, d_input, q)
    def renorm(t, q):
        rows = pl.ds(pl.multiple_of(t * tt, tt), tt)
        wide = xh[rows, :].astype(f32)
        a0 = (wide * rms_scale(wide)).astype(bf16)
        a[rows, :] = a0
        aT[:, rows] = a0.T
        return q
    pltpu.make_async_copy(x_in, xh, x_sem).wait()
    q = ops(q, 2, NB)
    lax.fori_loop(0, T // tt, renorm, 0)

    def first_layer(j, q):
        return block(0, j, 2 * GB, 2 * GB + T, NB + j, q, cfg["pace"][2])
    q = lax.fori_loop(0, NB, first_layer, q)
    if comm:
        lax.fori_loop(q, (LAST + 2) * n, op, 0)
        for r in range(LAST - RB + 2, LAST + 1):
            for s in range(n - 1):
                z = r - s
                b = z // 2 if z < 2 * ramp else z - ramp
                if z >= 0 and (z >= 2 * ramp or z % 2 == 0) and b < NBLK:
                    for d in range(2):
                        hop(r, s, d).wait_send()
        for d in range(2):
            for b in range(NBLK):
                pltpu.make_async_copy(S.at[pl.ds(0, CH), :], (own00, own01, own10, own11)[2 * (b // NB) + d].at[b % NB], own_sem.at[d, b]).wait()
    else:
        cps = [pltpu.make_async_copy(S.at[pl.ds(b * BR + d * CH, CH), :], (own00, own01, own10, own11)[2 * (b // NB) + d].at[b % NB], own_sem.at[d, b]) for d in range(2) for b in range(NBLK)]
        for c in cps: c.start()
        for c in cps: c.wait()


def k1(x, dy, wg, wu, wd, n, tt=512, tb=512, comm=True, cid=0, pace=(6, 7, 6)):
    T, D = x.shape
    F = wg.shape[2]
    NB = F // BW
    NBLK = 2 * NB
    H = D // (2 * n); CH = 3 * H
    GB = NB * 3 * D
    cfg = dict(n=n, T=T, D=D, F=F, tt=min(tt, T), tb=min(tb, T), comm=comm, pace=pace)
    any_ = pl.BlockSpec(memory_space=pl.ANY)
    flops = 18 * 2 * T * D * F
    return pl.pallas_call(
        functools.partial(kernel, cfg),
        out_shape=(jax.ShapeDtypeStruct((NB, CH, BW), bf16),) * 4 + (jax.ShapeDtypeStruct((8, 128), f32),),
        in_specs=[any_] * 5,
        out_specs=(any_,) * 4 + (pl.BlockSpec(memory_space=pltpu.VMEM),),
        scratch_shapes=[
            pltpu.VMEM((max(GB + NB * 2 * T, 2 * GB + 2 * T), BW), bf16),
            pltpu.VMEM((T, D), bf16), pltpu.VMEM((T, D), bf16), pltpu.VMEM((D, T), bf16), pltpu.VMEM((T, D), bf16),
            pltpu.VMEM((T, BW), bf16),
            pltpu.VMEM((2, D, F), bf16), pltpu.VMEM((2, D, F), bf16), pltpu.VMEM((2, F, D), bf16),
            pltpu.VMEM((2, RB * (n - 1), CH, BW), bf16),
            pltpu.SemaphoreType.DMA((8,)), pltpu.SemaphoreType.DMA, pltpu.SemaphoreType.DMA((2, NBLK)),
            pltpu.SemaphoreType.DMA((2, RB * (n - 1))), pltpu.SemaphoreType.DMA((2, RB * (n - 1))), pltpu.SemaphoreType.REGULAR((2,)),
        ],
        compiler_params=pltpu.CompilerParams(vmem_limit_bytes=67043328, collective_id=cid if comm else None, has_side_effects=True),
        cost_estimate=pl.CostEstimate(flops=flops, bytes_accessed=40 * 10**6, transcendentals=0),
        name="grads")(x, dy, wg, wu, wd)


def factor_kernel(n, count, sq, out, slots, send_sem, recv_sem):
    me = lax.axis_index("dp")
    barrier = pltpu.get_barrier_semaphore()
    peers = [lax.rem(me + p, n) for p in range(1, n)]
    for q in peers:
        pl.semaphore_signal(barrier, inc=1, device_id={"dp": q}, device_id_type=pl.DeviceIdType.MESH)
    slots[me] = sq[...]
    pl.semaphore_wait(barrier, n - 1)
    copies = [
        pltpu.make_async_remote_copy(
            src_ref=sq, dst_ref=slots.at[me], send_sem=send_sem.at[i], recv_sem=recv_sem.at[me],
            device_id={"dp": q}, device_id_type=pl.DeviceIdType.MESH)
        for i, q in enumerate(peers)]
    for c in copies:
        c.start()
    for i, q in enumerate(peers):
        pltpu.make_async_remote_copy(
            src_ref=sq, dst_ref=slots.at[q], send_sem=send_sem.at[i], recv_sem=recv_sem.at[q],
            device_id={"dp": q}, device_id_type=pl.DeviceIdType.MESH).wait_recv()
    total = slots[0]
    for i in range(1, n):
        total = total + slots[i]
    total = jnp.sum(jnp.sum(total, axis=0, keepdims=True), axis=1, keepdims=True)
    out[...] = jnp.broadcast_to(jnp.minimum(1.0, 0.5 * lax.rsqrt(total / count + 1e-30)), out.shape)
    for c in copies:
        c.wait_send()


def clip_factor(squares, count, n):
    vmem = pl.BlockSpec(memory_space=pltpu.VMEM)
    return pl.pallas_call(
        functools.partial(factor_kernel, n, float(count)),
        out_shape=jax.ShapeDtypeStruct(squares.shape, f32),
        in_specs=[vmem],
        out_specs=vmem,
        scratch_shapes=[pltpu.VMEM((n,) + squares.shape, f32), pltpu.SemaphoreType.DMA((n - 1,)), pltpu.SemaphoreType.DMA((n,))],
        compiler_params=pltpu.CompilerParams(collective_id=1, has_side_effects=True, vmem_limit_bytes=2**20),
        cost_estimate=pl.CostEstimate(flops=10**9, bytes_accessed=10**5, transcendentals=0),
        name="factor")(squares)


def adam_math(w, m, v, g):
    m = 0.9 * m + 0.1 * g
    v = 0.95 * v + 0.05 * g * g
    step = m * lax.rsqrt(v + 1e-8) + 0.1 * w
    return (w - 0.02 * step).astype(bf16), m, v


def adam_kernel(pieces, idx_ref, fac_ref, *refs):
    pays, ins, outs = refs[: len(pieces)], refs[len(pieces) : len(pieces) + 9], refs[-9:]
    factor = fac_ref[0:1, 0:1]
    def one(p):
        def step(k, at, g):
            new = adam_math(ins[k][at].astype(f32), ins[3 + k][at], ins[6 + k][at], g.astype(f32) * factor)
            for i in range(3):
                outs[3 * i + k][at] = new[i]
        hr = ins[2].shape[3]
        def block(j, _):
            cols = pl.ds(pl.multiple_of(j * BW, BW), BW)
            step(0, (0, 0, slice(None), cols), p[j, 0])
            step(1, (0, 0, slice(None), cols), p[j, 1])
            for cg in range(ins[2].shape[4] // BW):
                step(2, (0, j, 0, slice(None), slice(cg * BW, (cg + 1) * BW)), p[j, 2, cg * hr : (cg + 1) * hr])
            return 0
        lax.fori_loop(0, p.shape[0], block, 0)
    if len(pieces) == 1:
        one(pays[0])
    else:
        for i in range(len(pieces)):
            pl.when(pl.program_id(0) == i)(functools.partial(one, pays[i]))


def pick(values, i):
    out = values[0]
    for k in range(1, len(values)):
        out = jnp.where(i == k, values[k], out)
    return out


def adam_call(idx, factor, pieces, pays, ins, prev):
    nb = pays[0].shape[0]
    layer = lambda i: pick([l for l, _ in pieces], i)
    chunk = lambda i, idx: pick([idx[d] for _, d in pieces], i)
    rows = pl.BlockSpec((1, 1) + ins[0].shape[2:], lambda i, idx: (layer(i), chunk(i, idx), 0, 0))
    down = pl.BlockSpec((1, nb, 1) + ins[2].shape[3:], lambda i, idx: (layer(i), 0, chunk(i, idx), 0, 0))
    pay = pl.BlockSpec(pays[0].shape, lambda i, idx: (0, 0, 0, 0), pipeline_mode=pl.Buffered(1))
    specs = [rows, rows, down] * 3
    any_ = [] if prev is None else [pl.BlockSpec(memory_space=pl.ANY)] * 9
    k = len(pieces)
    size = k * pays[0].size
    return pl.pallas_call(
        functools.partial(adam_kernel, tuple(pieces)),
        grid_spec=pltpu.PrefetchScalarGridSpec(
            num_scalar_prefetch=1, grid=(k,), in_specs=[pl.BlockSpec((8, 128), lambda i, idx: (0, 0))] + [pay] * k + specs + any_, out_specs=specs),
        out_shape=[jax.ShapeDtypeStruct(x.shape, x.dtype) for x in ins],
        input_output_aliases={} if prev is None else {2 + k + 9 + i: i for i in range(9)},
        compiler_params=pltpu.CompilerParams(vmem_limit_bytes=62 * 2**20, dimension_semantics=("arbitrary",)),
        cost_estimate=pl.CostEstimate(flops=4 * 10**9 * k // 4, bytes_accessed=22 * size, transcendentals=size),
        name="adamw")(idx, factor, *pays, *ins, *([] if prev is None else prev))


def views(arrays, n):
    out = []
    for i, a in enumerate(arrays):
        L, r, c = a.shape
        out.append(a.reshape(L, 2 * n, r // (2 * n), c) if i % 3 < 2 else a.reshape(L, r // BW, 2 * n, BW // (2 * n), c))
    return out


def solution(mesh):
    n = mesh.shape["dp"]
    to = ([(i, (i + 1) % n) for i in range(n)], [(i, (i - 1) % n) for i in range(n)])

    def step(x, dy, *arrays):
        me = lax.axis_index("dp")
        own00, own01, own10, own11, squares = k1(x[0], dy[0], *arrays[:3], n)
        _, _, F = arrays[0].shape
        ins = views(arrays, n)
        count = sum(w.size for w in arrays[:3])
        pieces = [(1, 0), (1, 1), (0, 0), (0, 1)]
        pays = [o.reshape(F // BW, 3, o.shape[1] // 3, BW) for o in (own00, own01, own10, own11)]
        factor, outs = None, None
        for s in range(n):
            coming = []
            if s < n - 1:
                for i, (l, d) in enumerate(pieces):
                    coming.append(lax.ppermute(pays[i], "dp", to[d]))
            if factor is None:
                factor = clip_factor(squares, count, n)
            c0, c1 = lax.rem(me - s + n, n), lax.rem(me + s, n)
            idx = jnp.stack([2 * c0, 2 * c1 + 1]).astype(jnp.int32)
            if s < n - 1:
                outs = adam_call(idx, factor, pieces, pays, ins, outs)
            else:
                outs = adam_call(idx, factor, pieces[:2], pays[:2], ins, outs)
                outs = adam_call(idx, factor, pieces[2:], pays[2:], ins, outs)
            pays = coming
        return tuple(o.reshape(w.shape) for o, w in zip(outs, arrays))

    step = jax.shard_map(
        step,
        mesh=mesh,
        in_specs=(P(("rep", "dp"), None, None),) * 2 + (P(None, None, None),) * 9,
        out_specs=(P("rep", None, None),) * 9,
        check_vma=False,
    )
    return step
```

```python
import functools

import jax
import jax.numpy as jnp
from jax import lax
from jax.experimental import pallas as pl
from jax.experimental.pallas import tpu as pltpu
from jax.sharding import PartitionSpec as P


BW = 256
RB = 3
f32, bf16 = jnp.float32, jnp.bfloat16
NT = (((1,), (1,)), ((), ()))
TN = (((0,), (0,)), ((), ()))


def mm(a, b, dims=(((1,), (0,)), ((), ()))):
    return lax.dot_general(a, b, dims, preferred_element_type=f32)


def rms_scale(wide):
    return lax.rsqrt(jnp.mean(wide * wide, -1, keepdims=True) + 1e-6)


def sigmoid(x):
    return 0.5 * jnp.tanh(0.5 * x) + 0.5


def kernel(cfg, x_in, dy_in, wg_in, wu_in, wd_in, own00, own01, own10, own11, got0, got1, ss, S, xh, a, aT, dh, hid, wg, wu, wd, recv,
           load_sem, x_sem, own_sem, send_sem, recv_sem, credit, got_send, got_recv):
    n, T, D, F, tt, tb, comm = cfg["n"], cfg["T"], cfg["D"], cfg["F"], cfg["tt"], cfg["tb"], cfg["comm"]
    NB = F // BW
    NBLK = 2 * NB
    H = D // (2 * n)
    CH = 3 * H
    BR = 3 * D
    GB = NB * BR
    hr = BW // (2 * n)
    ncg = D // BW
    ramp = max(NBLK - 4, 1)
    start = lambda b: jnp.where(b <= ramp, 2 * b, b + ramp)
    LAST = NBLK - 1 + ramp + n - 2
    me = lax.axis_index("dp")
    right, left = lax.rem(me + 1, n), lax.rem(me + n - 1, n)

    loads = [pltpu.make_async_copy(s, d, load_sem.at[i]) for i, (s, d) in enumerate((
        (x_in, xh), (wg_in.at[0], wg.at[0]), (wu_in.at[0], wu.at[0]), (wd_in.at[0], wd.at[0]), (dy_in, dh),
        (wg_in.at[1], wg.at[1]), (wu_in.at[1], wu.at[1]), (wd_in.at[1], wd.at[1])))]
    for c in loads[:3]:
        c.start()
    if comm:
        barrier = pltpu.get_barrier_semaphore()
        for nb in (left, right):
            pl.semaphore_signal(barrier, inc=1, device_id={"dp": nb}, device_id_type=pl.DeviceIdType.MESH)
    ss[...] = jnp.zeros_like(ss)

    def chunk_row(b, c, d):
        return pl.multiple_of(b * BR + (2 * c + d) * CH, 16)

    def chunk_of(s, d):
        return lax.rem(me + 2 * n - 1 - s, n) if d == 0 else lax.rem(me + 1 + s, n)

    def block_of(r, s):
        z = r - s
        b = jnp.where(z < 2 * ramp, lax.div(z, 2), z - ramp)
        return b, (z >= 0) & ((z >= 2 * ramp) | (lax.rem(z, 2) == 0)) & (b < NBLK)

    def hop(r, s, d):
        b, _ = block_of(r, s)
        slot = lax.rem(r, RB) * (n - 1) + s
        return pltpu.make_async_remote_copy(
            src_ref=S.at[pl.ds(chunk_row(b, chunk_of(s, d), d), CH), :], dst_ref=recv.at[d, slot],
            send_sem=send_sem.at[d, slot], recv_sem=recv_sem.at[d, slot],
            device_id={"dp": right if d == 0 else left}, device_id_type=pl.DeviceIdType.MESH)

    def arrival(d, slot):
        return pltpu.make_async_remote_copy(
            src_ref=recv.at[d, slot], dst_ref=recv.at[d, slot], send_sem=send_sem.at[d, slot], recv_sem=recv_sem.at[d, slot],
            device_id={"dp": right if d == 0 else left}, device_id_type=pl.DeviceIdType.MESH)

    def onward(k, d):
        return pltpu.make_async_remote_copy(
            src_ref=S.at[pl.ds(chunk_row(k, me, d), CH), :], dst_ref=(got0, got1)[d].at[k],
            send_sem=got_send.at[d, k], recv_sem=got_recv.at[d, k],
            device_id={"dp": right if d == 0 else left}, device_id_type=pl.DeviceIdType.MESH)

    def op(q, _):
        r, s = lax.div(q, n), lax.rem(q, n)
        b, live = block_of(r, s)
        @pl.when((s == 0) & (r >= RB) & (r <= LAST))
        def _():
            pl.semaphore_wait(credit.at[0], 1)
            pl.semaphore_wait(credit.at[1], 1)
        @pl.when(live & (s >= 1))
        def _():
            slot = lax.rem(r + RB - 1, RB) * (n - 1) + s - 1
            for d in range(2):
                arrival(d, slot).wait_recv()
                rows = pl.ds(chunk_row(b, chunk_of(s, d), d), CH)
                total = (S[rows, :].astype(f32) + recv[d, slot].astype(f32)).astype(bf16)
                S[rows, :] = total
                @pl.when(s == n - 1)
                def _():
                    t = total.astype(f32)
                    t = t * t
                    ss[...] += functools.reduce(jnp.add, [t[i * 8:(i + 1) * 8, h * 128:(h + 1) * 128] for i in range(CH // 8) for h in range(BW // 128)])
        @pl.when(live & (s == n - 1))
        def _():
            for d in range(2):
                rows = pl.ds(chunk_row(b, me, d), CH)
                @pl.when(b < NB)
                def _():
                    pltpu.make_async_copy(S.at[rows, :], (own00, own01)[d].at[b], own_sem.at[d, b]).start()
                @pl.when(b >= NB)
                def _():
                    pltpu.make_async_copy(S.at[rows, :], (own10, own11)[d].at[b - NB], own_sem.at[d, b]).start()
        _, before = block_of(r - RB, s)
        @pl.when((s <= n - 2) & (r >= RB) & before)
        def _():
            for d in range(2):
                hop(r - RB, s, d).wait_send()
        @pl.when(live & (s <= n - 2))
        def _():
            for d in range(2):
                hop(r, s, d).start()
        for when, blocks in ((LAST - 1, range(0, 1)), (LAST, range(1, 3)), (LAST + 1, range(3, NB))):
            @pl.when((s == n - 1) & (r == when))
            def _():
                for k in blocks:
                    if k < NB:
                        for d in range(2):
                            onward(k, d).start()
        @pl.when((s == n - 1) & (r >= 1) & (r <= LAST - RB + 1))
        def _():
            pl.semaphore_signal(credit.at[0], inc=1, device_id={"dp": left}, device_id_type=pl.DeviceIdType.MESH)
            pl.semaphore_signal(credit.at[1], inc=1, device_id={"dp": right}, device_id_type=pl.DeviceIdType.MESH)
        return 0

    def ops(q, count, ready):
        if not comm:
            return q
        limit = n * start(ready)
        end = jnp.where(q + count < limit, q + count, limit)
        lax.fori_loop(q, end, op, 0)
        return end

    loads[0].wait()
    loads[3].start()
    loads[1].wait()
    loads[2].wait()
    def fwd(t, _):
        rows = pl.ds(pl.multiple_of(t * tt, tt), tt)
        xw = xh[rows, :].astype(f32)
        at = (xw * rms_scale(xw)).astype(bf16)
        for j in range(NB):
            cols = slice(j * BW, (j + 1) * BW)
            g = mm(at, wg[0, :, cols])
            u = mm(at, wu[0, :, cols])
            S[pl.ds(pl.multiple_of(GB + j * T + t * tt, 16), tt), :] = (g * sigmoid(g) * u).astype(bf16)
        return 0
    lax.fori_loop(0, T // tt, fwd, 0)
    loads[3].wait()
    for c in loads[4:]:
        c.start()
    def fwd_down(t, _):
        rows = pl.ds(pl.multiple_of(t * tt, tt), tt)
        hidden = jnp.concatenate([S[pl.ds(pl.multiple_of(GB + j * T + t * tt, 16), tt), :] for j in range(NB)], axis=1)
        h = (xh[rows, :].astype(f32) + mm(hidden, wd[0]).astype(bf16).astype(f32)).astype(bf16)
        xh[rows, :] = h
        hw = h.astype(f32)
        a1 = (hw * rms_scale(hw)).astype(bf16)
        a[rows, :] = a1
        aT[:, rows] = a1.T
        return 0
    lax.fori_loop(0, T // tt, fwd_down, 0)

    def block(l, j, dg0, du0, b, q, pace):
        cols = pl.ds(pl.multiple_of(j * BW, BW), BW)
        q = ops(q, pace, b)
        def tokens(t, q):
            rows = pl.ds(pl.multiple_of(t * tb, tb), tb)
            at = a[rows, :]
            g = mm(at, wg[l, :, cols])
            u = mm(at, wu[l, :, cols])
            dhid = mm(dh[rows, :], wd[l, cols, :], NT).astype(bf16).astype(f32)
            sg = sigmoid(g)
            s = g * sg
            hid[rows, :] = (s * u).astype(bf16)
            S[pl.ds(pl.multiple_of(du0 + t * tb, 16), tb), :] = (dhid * s).astype(bf16)
            S[pl.ds(pl.multiple_of(dg0 + t * tb, 16), tb), :] = (dhid * u * (sg + s * (1.0 - sg))).astype(bf16)
            return q
        q = lax.fori_loop(0, T // tb, tokens, q, unroll=True)
        base = b * BR
        def gate_up(w, k):
            for e in range(2 * n):
                S[pl.ds(pl.multiple_of(base + e * CH + k * H, 16), H), :] = w[e * H:(e + 1) * H]
        def down(w):
            for e in range(2 * n):
                for cg in range(ncg):
                    S[pl.ds(pl.multiple_of(base + e * CH + 2 * H + cg * hr, 16), hr), :] = w[e * hr:(e + 1) * hr, cg * BW:(cg + 1) * BW]
        dgv = lambda: S[pl.ds(pl.multiple_of(dg0, 16), T), :]
        duv = lambda: S[pl.ds(pl.multiple_of(du0, 16), T), :]
        q = ops(q, pace, b)
        w = mm(aT[...], jnp.concatenate([dgv(), duv()], axis=1)).astype(bf16)
        gate_up(w[:, :BW], 0)
        gate_up(w[:, BW:], 1)
        down(mm(hid[...], dh[...], TN).astype(bf16))
        return q

    for c in loads[4:]:
        c.wait()
    def last_layer(j, q):
        return block(1, j, GB + j * 2 * T, GB + j * 2 * T + T, j, q, jnp.where(j <= 2, n, cfg["pace"][0]))
    if comm:
        pl.semaphore_wait(barrier, 2)
    q = lax.fori_loop(0, NB, last_layer, 0)

    def d_input(t, q):
        q = ops(q, cfg["pace"][1], NB)
        rows = pl.ds(pl.multiple_of(t * tt, tt), tt)
        dg = jnp.concatenate([S[pl.ds(pl.multiple_of(GB + j * 2 * T + t * tt, 16), tt), :] for j in range(NB)], axis=1)
        du = jnp.concatenate([S[pl.ds(pl.multiple_of(GB + j * 2 * T + T + t * tt, 16), tt), :] for j in range(NB)], axis=1)
        da = (mm(dg, wg[1], NT).astype(bf16).astype(f32) + mm(du, wu[1], NT).astype(bf16).astype(f32)).astype(bf16).astype(f32)
        wide = xh[rows, :].astype(f32)
        scale = rms_scale(wide)
        dot = jnp.sum(da * wide, -1, keepdims=True)
        dw = da * scale - wide * (scale * scale * scale * dot * (1.0 / D))
        dh[rows, :] = (dh[rows, :].astype(f32) + dw.astype(bf16).astype(f32)).astype(bf16)
        pltpu.make_async_copy(x_in.at[rows, :], xh.at[rows, :], x_sem).start()
        return q
    q = lax.fori_loop(0, T // tt, d_input, q)
    def renorm(t, q):
        rows = pl.ds(pl.multiple_of(t * tt, tt), tt)
        wide = xh[rows, :].astype(f32)
        a0 = (wide * rms_scale(wide)).astype(bf16)
        a[rows, :] = a0
        aT[:, rows] = a0.T
        return q
    pltpu.make_async_copy(x_in, xh, x_sem).wait()
    q = ops(q, 2, NB)
    lax.fori_loop(0, T // tt, renorm, 0)

    def first_layer(j, q):
        return block(0, j, 2 * GB, 2 * GB + T, NB + j, q, cfg["pace"][2])
    q = lax.fori_loop(0, NB, first_layer, q)
    if comm:
        lax.fori_loop(q, (LAST + 2) * n, op, 0)
        for r in range(LAST - RB + 2, LAST + 1):
            for s in range(n - 1):
                z = r - s
                b = z // 2 if z < 2 * ramp else z - ramp
                if z >= 0 and (z >= 2 * ramp or z % 2 == 0) and b < NBLK:
                    for d in range(2):
                        hop(r, s, d).wait_send()
        for d in range(2):
            for k in range(NB):
                onward(k, d).wait_recv()
                onward(k, d).wait_send()
        for d in range(2):
            for b in range(NBLK):
                pltpu.make_async_copy(S.at[pl.ds(0, CH), :], (own00, own01, own10, own11)[2 * (b // NB) + d].at[b % NB], own_sem.at[d, b]).wait()
    else:
        cps = [pltpu.make_async_copy(S.at[pl.ds(b * BR + d * CH, CH), :], (own00, own01, own10, own11)[2 * (b // NB) + d].at[b % NB], own_sem.at[d, b]) for d in range(2) for b in range(NBLK)]
        for c in cps: c.start()
        for c in cps: c.wait()


def k1(x, dy, wg, wu, wd, n, tt=512, tb=512, comm=True, cid=0, pace=(6, 7, 6)):
    T, D = x.shape
    F = wg.shape[2]
    NB = F // BW
    NBLK = 2 * NB
    H = D // (2 * n); CH = 3 * H
    GB = NB * 3 * D
    cfg = dict(n=n, T=T, D=D, F=F, tt=min(tt, T), tb=min(tb, T), comm=comm, pace=pace)
    any_ = pl.BlockSpec(memory_space=pl.ANY)
    flops = 18 * 2 * T * D * F
    return pl.pallas_call(
        functools.partial(kernel, cfg),
        out_shape=(jax.ShapeDtypeStruct((NB, CH, BW), bf16),) * 6 + (jax.ShapeDtypeStruct((8, 128), f32),),
        in_specs=[any_] * 5,
        out_specs=(any_,) * 6 + (pl.BlockSpec(memory_space=pltpu.VMEM),),
        scratch_shapes=[
            pltpu.VMEM((max(GB + NB * 2 * T, 2 * GB + 2 * T), BW), bf16),
            pltpu.VMEM((T, D), bf16), pltpu.VMEM((T, D), bf16), pltpu.VMEM((D, T), bf16), pltpu.VMEM((T, D), bf16),
            pltpu.VMEM((T, BW), bf16),
            pltpu.VMEM((2, D, F), bf16), pltpu.VMEM((2, D, F), bf16), pltpu.VMEM((2, F, D), bf16),
            pltpu.VMEM((2, RB * (n - 1), CH, BW), bf16),
            pltpu.SemaphoreType.DMA((8,)), pltpu.SemaphoreType.DMA, pltpu.SemaphoreType.DMA((2, NBLK)),
            pltpu.SemaphoreType.DMA((2, RB * (n - 1))), pltpu.SemaphoreType.DMA((2, RB * (n - 1))), pltpu.SemaphoreType.REGULAR((2,)),
            pltpu.SemaphoreType.DMA((2, NB)), pltpu.SemaphoreType.DMA((2, NB)),
        ],
        compiler_params=pltpu.CompilerParams(vmem_limit_bytes=67043328, collective_id=cid if comm else None, has_side_effects=True),
        cost_estimate=pl.CostEstimate(flops=flops, bytes_accessed=40 * 10**6, transcendentals=0),
        name="grads")(x, dy, wg, wu, wd)


def factor_kernel(n, count, sq, out, slots, send_sem, recv_sem):
    me = lax.axis_index("dp")
    barrier = pltpu.get_barrier_semaphore()
    peers = [lax.rem(me + p, n) for p in range(1, n)]
    for q in peers:
        pl.semaphore_signal(barrier, inc=1, device_id={"dp": q}, device_id_type=pl.DeviceIdType.MESH)
    slots[me] = sq[...]
    pl.semaphore_wait(barrier, n - 1)
    copies = [
        pltpu.make_async_remote_copy(
            src_ref=sq, dst_ref=slots.at[me], send_sem=send_sem.at[i], recv_sem=recv_sem.at[me],
            device_id={"dp": q}, device_id_type=pl.DeviceIdType.MESH)
        for i, q in enumerate(peers)]
    for c in copies:
        c.start()
    for i, q in enumerate(peers):
        pltpu.make_async_remote_copy(
            src_ref=sq, dst_ref=slots.at[q], send_sem=send_sem.at[i], recv_sem=recv_sem.at[q],
            device_id={"dp": q}, device_id_type=pl.DeviceIdType.MESH).wait_recv()
    total = slots[0]
    for i in range(1, n):
        total = total + slots[i]
    total = jnp.sum(jnp.sum(total, axis=0, keepdims=True), axis=1, keepdims=True)
    out[...] = jnp.broadcast_to(jnp.minimum(1.0, 0.5 * lax.rsqrt(total / count + 1e-30)), out.shape)
    for c in copies:
        c.wait_send()


def clip_factor(squares, count, n):
    vmem = pl.BlockSpec(memory_space=pltpu.VMEM)
    return pl.pallas_call(
        functools.partial(factor_kernel, n, float(count)),
        out_shape=jax.ShapeDtypeStruct(squares.shape, f32),
        in_specs=[vmem],
        out_specs=vmem,
        scratch_shapes=[pltpu.VMEM((n,) + squares.shape, f32), pltpu.SemaphoreType.DMA((n - 1,)), pltpu.SemaphoreType.DMA((n,))],
        compiler_params=pltpu.CompilerParams(collective_id=1, has_side_effects=True, vmem_limit_bytes=2**20),
        cost_estimate=pl.CostEstimate(flops=10**9, bytes_accessed=10**5, transcendentals=0),
        name="factor")(squares)


def adam_math(w, m, v, g):
    m = 0.9 * m + 0.1 * g
    v = 0.95 * v + 0.05 * g * g
    step = m * lax.rsqrt(v + 1e-8) + 0.1 * w
    return (w - 0.02 * step).astype(bf16), m, v


def adam_kernel(layers, idx_ref, fac_ref, *refs):
    k = len(layers)
    pays, ins, outs = refs[:k], refs[k : k + 9], refs[-17:-8]
    gbuf, wbuf, wdown, fbuf, fdown, gsem, isem, osem = refs[-8:]
    factor = fac_ref[0:1, 0:1]

    def place(i, a):
        which, kind = a // 3, a % 3
        if which == 0:
            return wdown.at[i] if kind == 2 else wbuf.at[i, kind]
        return fdown.at[i, which - 1] if kind == 2 else fbuf.at[i, which - 1, kind]

    def rows(arrays, i, a):
        return arrays[a].at[layers[i], :, idx_ref[i]] if a % 3 == 2 else arrays[a].at[layers[i], idx_ref[i]]

    loads = [[pltpu.make_async_copy(pays[i], gbuf.at[i], gsem.at[i])] + [pltpu.make_async_copy(rows(ins, i, a), place(i, a), isem.at[i, a]) for a in range(9)] for i in range(k)]
    stores = [[pltpu.make_async_copy(place(i, a), rows(outs, i, a), osem.at[i, a]) for a in range(9)] for i in range(k)]
    for piece in loads:
        for c in piece:
            c.start()
    hr = wdown.shape[2]
    for i in range(k):
        for c in loads[i]:
            c.wait()
        def step(w, m, v, at, g):
            new = adam_math(w[at].astype(f32), m[at], v[at], g.astype(f32) * factor)
            for ref, value in zip((w, m, v), new, strict=True):
                ref[at] = value
        def block(j, _):
            cols = pl.ds(pl.multiple_of(j * BW, BW), BW)
            for kind in range(2):
                step(wbuf.at[i, kind], fbuf.at[i, 0, kind], fbuf.at[i, 1, kind], (slice(None), cols), gbuf[i, j, kind])
            for cg in range(wdown.shape[3] // BW):
                at = (j, slice(None), slice(cg * BW, (cg + 1) * BW))
                step(wdown.at[i], fdown.at[i, 0], fdown.at[i, 1], at, gbuf[i, j, 2, cg * hr : (cg + 1) * hr])
            return 0
        lax.fori_loop(0, gbuf.shape[1], block, 0)
        for c in stores[i]:
            c.start()
    for piece in stores:
        for c in piece:
            c.wait()


def adam_call(factor, pieces, ins, prev):
    k = len(pieces)
    layers = tuple(l for l, _, _ in pieces)
    idx = jnp.stack([c for _, c, _ in pieces]).astype(jnp.int32)
    pays = [g for _, _, g in pieces]
    hbm = pl.BlockSpec(memory_space=pl.ANY)
    kept = [] if prev is None else list(prev)
    size = k * pays[0].size
    rows, down = ins[0].shape[2:], (ins[2].shape[1],) + ins[2].shape[3:]
    return pl.pallas_call(
        functools.partial(adam_kernel, layers),
        grid_spec=pltpu.PrefetchScalarGridSpec(
            num_scalar_prefetch=1, grid=(1,),
            in_specs=[pl.BlockSpec((8, 128), lambda i, idx: (0, 0))] + [hbm] * (k + 9 + len(kept)),
            out_specs=[hbm] * 9,
            scratch_shapes=[
                pltpu.VMEM((k,) + pays[0].shape, bf16), pltpu.VMEM((k, 2) + rows, bf16), pltpu.VMEM((k,) + down, bf16),
                pltpu.VMEM((k, 2, 2) + rows, f32), pltpu.VMEM((k, 2) + down, f32),
                pltpu.SemaphoreType.DMA((k,)), pltpu.SemaphoreType.DMA((k, 9)), pltpu.SemaphoreType.DMA((k, 9))]),
        out_shape=[jax.ShapeDtypeStruct(x.shape, x.dtype) for x in ins],
        input_output_aliases={} if prev is None else {2 + k + 9 + i: i for i in range(9)},
        compiler_params=pltpu.CompilerParams(vmem_limit_bytes=62 * 2**20),
        cost_estimate=pl.CostEstimate(flops=10**9 * k, bytes_accessed=22 * size, transcendentals=size),
        name="adamw")(idx, factor, *pays, *ins, *kept)


def views(arrays, n):
    out = []
    for i, a in enumerate(arrays):
        L, r, c = a.shape
        out.append(a.reshape(L, 2 * n, r // (2 * n), c) if i % 3 < 2 else a.reshape(L, r // BW, 2 * n, BW // (2 * n), c))
    return out


def solution(mesh):
    n = mesh.shape["dp"]
    to = ([(i, (i + 1) % n) for i in range(n)], [(i, (i - 1) % n) for i in range(n)])

    def step(x, dy, *arrays):
        me = lax.axis_index("dp")
        *sums, squares = k1(x[0], dy[0], *arrays[:3], n)
        _, _, F = arrays[0].shape
        ins = views(arrays, n)
        count = sum(w.size for w in arrays[:3])
        last, first, came = ([o.reshape(F // BW, 3, o.shape[1] // 3, BW) for o in sums[i : i + 2]] for i in (0, 2, 4))

        def pieces(layer, pays, hops):
            return [(layer, 2 * lax.rem(me - hops + n, n), pays[0]), (layer, 2 * lax.rem(me + hops, n) + 1, pays[1])]

        waiting = pieces(1, last, 0) + pieces(0, first, 0) + pieces(1, came, 1)
        outs, last = None, came
        for s in range(1, n):
            ahead = []
            for d in range(2):
                first[d] = lax.ppermute(first[d], "dp", to[d])
            if s < n - 1:
                for d in range(2):
                    ahead.append(lax.ppermute(last[d], "dp", to[d]))
            if s == 1:
                factor = clip_factor(squares, count, n)
            else:
                outs = adam_call(factor, waiting, ins, outs)
                waiting = []
            waiting = waiting + pieces(0, first, s) + (pieces(1, ahead, s + 1) if ahead else [])
            first, last = list(first), ahead
        outs = adam_call(factor, waiting, ins, outs)
        return tuple(o.reshape(w.shape) for o, w in zip(outs, arrays))

    step = jax.shard_map(
        step,
        mesh=mesh,
        in_specs=(P(("rep", "dp"), None, None),) * 2 + (P(None, None, None),) * 9,
        out_specs=(P("rep", None, None),) * 9,
        check_vma=False,
    )
    return step
```

```python
import functools

import jax
import jax.numpy as jnp
from jax import lax
from jax.experimental import pallas as pl
from jax.experimental.pallas import tpu as pltpu
from jax.sharding import PartitionSpec as P


BW = 256
RB = 3
f32, bf16 = jnp.float32, jnp.bfloat16
NT = (((1,), (1,)), ((), ()))
TN = (((0,), (0,)), ((), ()))


def mm(a, b, dims=(((1,), (0,)), ((), ()))):
    return lax.dot_general(a, b, dims, preferred_element_type=f32)


def rms_scale(wide):
    return lax.rsqrt(jnp.mean(wide * wide, -1, keepdims=True) + 1e-6)


def sigmoid(x):
    return 0.5 * jnp.tanh(0.5 * x) + 0.5


def kernel(cfg, x_in, dy_in, wg_in, wu_in, wd_in, own00, own01, own10, own11, got0, got1, factor, S, xh, a, aT, dh, hid, wg, wu, wd, recv,
           load_sem, x_sem, own_sem, send_sem, recv_sem, credit, got_send, got_recv, ss, squares, sq_send, sq_recv):
    n, T, D, F, tt, tb, comm = cfg["n"], cfg["T"], cfg["D"], cfg["F"], cfg["tt"], cfg["tb"], cfg["comm"]
    NB = F // BW
    NBLK = 2 * NB
    H = D // (2 * n)
    CH = 3 * H
    BR = 3 * D
    GB = NB * BR
    hr = BW // (2 * n)
    ncg = D // BW
    gap = cfg["gap"]
    ramp = max(NBLK - cfg["quick"], NB)
    def start(b):
        return jnp.where(b < NB, 2 * b, jnp.where(b <= ramp, 2 * b + gap, b + ramp + gap))
    LAST = NBLK - 1 + ramp + gap + n - 2
    ahead = ((LAST - 2, range(0, min(1, NB))), (LAST - 1, range(1, min(3, NB))), (LAST, range(3, min(6, NB))))
    me = lax.axis_index("dp")
    right, left = lax.rem(me + 1, n), lax.rem(me + n - 1, n)
    peers = [lax.rem(me + i, n) for i in range(1, n)]

    loads = [pltpu.make_async_copy(s, d, load_sem.at[i]) for i, (s, d) in enumerate((
        (x_in, xh), (wg_in.at[0], wg.at[0]), (wu_in.at[0], wu.at[0]), (wd_in.at[0], wd.at[0]), (dy_in, dh),
        (wg_in.at[1], wg.at[1]), (wu_in.at[1], wu.at[1]), (wd_in.at[1], wd.at[1])))]
    for c in loads[:3]:
        c.start()
    if comm:
        barrier = pltpu.get_barrier_semaphore()
        for p in peers:
            pl.semaphore_signal(barrier, inc=1, device_id={"dp": p}, device_id_type=pl.DeviceIdType.MESH)
    ss[...] = jnp.zeros_like(ss)

    def chunk_row(b, c, d):
        return pl.multiple_of(b * BR + (2 * c + d) * CH, 16)

    def chunk_of(s, d):
        return lax.rem(me + 2 * n - 1 - s, n) if d == 0 else lax.rem(me + 1 + s, n)

    def block_of(r, s):
        z = r - s
        y = z - gap
        b = jnp.where(z < 2 * NB, lax.div(z, 2), jnp.where(y < 2 * ramp, lax.div(y, 2), y - ramp))
        early = (z >= 0) & (z < 2 * NB) & (lax.rem(z, 2) == 0)
        late = (y >= 2 * NB) & ((y >= 2 * ramp) | (lax.rem(y, 2) == 0))
        return b, (early | late) & (b < NBLK)

    def hop(r, s, d):
        b, _ = block_of(r, s)
        slot = lax.rem(r, RB) * (n - 1) + s
        return pltpu.make_async_remote_copy(
            src_ref=S.at[pl.ds(chunk_row(b, chunk_of(s, d), d), CH), :], dst_ref=recv.at[d, slot],
            send_sem=send_sem.at[d, slot], recv_sem=recv_sem.at[d, slot],
            device_id={"dp": right if d == 0 else left}, device_id_type=pl.DeviceIdType.MESH)

    def arrival(d, slot):
        return pltpu.make_async_remote_copy(
            src_ref=recv.at[d, slot], dst_ref=recv.at[d, slot], send_sem=send_sem.at[d, slot], recv_sem=recv_sem.at[d, slot],
            device_id={"dp": right if d == 0 else left}, device_id_type=pl.DeviceIdType.MESH)

    def onward(k, d):
        return pltpu.make_async_remote_copy(
            src_ref=S.at[pl.ds(chunk_row(k, me, d), CH), :], dst_ref=(got0, got1)[d].at[k],
            send_sem=got_send.at[d, k], recv_sem=got_recv.at[d, k],
            device_id={"dp": right if d == 0 else left}, device_id_type=pl.DeviceIdType.MESH)

    def op(q, _):
        r, s = lax.div(q, n), lax.rem(q, n)
        b, live = block_of(r, s)
        @pl.when((s == 0) & (r >= RB) & (r <= LAST))
        def _():
            pl.semaphore_wait(credit.at[0], 1)
            pl.semaphore_wait(credit.at[1], 1)
        @pl.when(live & (s >= 1))
        def _():
            slot = lax.rem(r + RB - 1, RB) * (n - 1) + s - 1
            for d in range(2):
                arrival(d, slot).wait_recv()
                rows = pl.ds(chunk_row(b, chunk_of(s, d), d), CH)
                total = (S[rows, :].astype(f32) + recv[d, slot].astype(f32)).astype(bf16)
                S[rows, :] = total
                @pl.when(s == n - 1)
                def _():
                    t = total.astype(f32)
                    t = t * t
                    ss[...] += functools.reduce(jnp.add, [t[i * 8:(i + 1) * 8, h * 128:(h + 1) * 128] for i in range(CH // 8) for h in range(BW // 128)])
        @pl.when(live & (s == n - 1))
        def _():
            for d in range(2):
                rows = pl.ds(chunk_row(b, me, d), CH)
                @pl.when(b < NB)
                def _():
                    pltpu.make_async_copy(S.at[rows, :], (own00, own01)[d].at[b], own_sem.at[d, b]).start()
                @pl.when(b >= NB)
                def _():
                    pltpu.make_async_copy(S.at[rows, :], (own10, own11)[d].at[b - NB], own_sem.at[d, b]).start()
        _, before = block_of(r - RB, s)
        @pl.when((s <= n - 2) & (r >= RB) & before)
        def _():
            for d in range(2):
                hop(r - RB, s, d).wait_send()
        @pl.when(live & (s <= n - 2))
        def _():
            for d in range(2):
                hop(r, s, d).start()
        for when, blocks in ahead:
            @pl.when((s == n - 1) & (r == when))
            def _():
                for k in blocks:
                    for d in range(2):
                        onward(k, d).start()
        @pl.when((s == n - 1) & (r >= 1) & (r <= LAST - RB + 1))
        def _():
            pl.semaphore_signal(credit.at[0], inc=1, device_id={"dp": left}, device_id_type=pl.DeviceIdType.MESH)
            pl.semaphore_signal(credit.at[1], inc=1, device_id={"dp": right}, device_id_type=pl.DeviceIdType.MESH)
        return 0

    def ops(q, count, ready):
        if not comm:
            return q
        limit = n * start(ready)
        end = jnp.where(q + count < limit, q + count, limit)
        lax.fori_loop(q, end, op, 0)
        return end

    loads[0].wait()
    loads[3].start()
    loads[1].wait()
    loads[2].wait()
    def fwd(t, _):
        rows = pl.ds(pl.multiple_of(t * tt, tt), tt)
        xw = xh[rows, :].astype(f32)
        at = (xw * rms_scale(xw)).astype(bf16)
        for j in range(NB):
            cols = slice(j * BW, (j + 1) * BW)
            g = mm(at, wg[0, :, cols])
            u = mm(at, wu[0, :, cols])
            S[pl.ds(pl.multiple_of(GB + j * T + t * tt, 16), tt), :] = (g * sigmoid(g) * u).astype(bf16)
        return 0
    lax.fori_loop(0, T // tt, fwd, 0)
    loads[3].wait()
    for c in loads[4:]:
        c.start()
    def fwd_down(t, _):
        rows = pl.ds(pl.multiple_of(t * tt, tt), tt)
        hidden = jnp.concatenate([S[pl.ds(pl.multiple_of(GB + j * T + t * tt, 16), tt), :] for j in range(NB)], axis=1)
        h = (xh[rows, :].astype(f32) + mm(hidden, wd[0]).astype(bf16).astype(f32)).astype(bf16)
        xh[rows, :] = h
        hw = h.astype(f32)
        a1 = (hw * rms_scale(hw)).astype(bf16)
        a[rows, :] = a1
        aT[:, rows] = a1.T
        return 0
    lax.fori_loop(0, T // tt, fwd_down, 0)

    def block(l, j, dg0, du0, b, q, pace, pace2):
        cols = pl.ds(pl.multiple_of(j * BW, BW), BW)
        q = ops(q, pace, b)
        def tokens(t, q):
            rows = pl.ds(pl.multiple_of(t * tb, tb), tb)
            at = a[rows, :]
            g = mm(at, wg[l, :, cols])
            u = mm(at, wu[l, :, cols])
            dhid = mm(dh[rows, :], wd[l, cols, :], NT).astype(bf16).astype(f32)
            sg = sigmoid(g)
            s = g * sg
            hid[rows, :] = (s * u).astype(bf16)
            S[pl.ds(pl.multiple_of(du0 + t * tb, 16), tb), :] = (dhid * s).astype(bf16)
            S[pl.ds(pl.multiple_of(dg0 + t * tb, 16), tb), :] = (dhid * u * (sg + s * (1.0 - sg))).astype(bf16)
            return q
        q = lax.fori_loop(0, T // tb, tokens, q, unroll=True)
        base = b * BR
        def gate_up(w, k):
            for e in range(2 * n):
                S[pl.ds(pl.multiple_of(base + e * CH + k * H, 16), H), :] = w[e * H:(e + 1) * H]
        def down(w):
            for e in range(2 * n):
                for cg in range(ncg):
                    S[pl.ds(pl.multiple_of(base + e * CH + 2 * H + cg * hr, 16), hr), :] = w[e * hr:(e + 1) * hr, cg * BW:(cg + 1) * BW]
        dgv = lambda: S[pl.ds(pl.multiple_of(dg0, 16), T), :]
        duv = lambda: S[pl.ds(pl.multiple_of(du0, 16), T), :]
        q = ops(q, pace2, b)
        w = mm(aT[...], jnp.concatenate([dgv(), duv()], axis=1)).astype(bf16)
        gate_up(w[:, :BW], 0)
        gate_up(w[:, BW:], 1)
        down(mm(hid[...], dh[...], TN).astype(bf16))
        return q

    for c in loads[4:]:
        c.wait()
    def last_layer(j, q):
        return block(1, j, GB + j * 2 * T, GB + j * 2 * T + T, j, q, jnp.where(j <= 2, n, cfg["pace"][0]), jnp.where(j <= 2, n, cfg["pace"][1]))
    if comm:
        pl.semaphore_wait(barrier, n - 1)
    q = lax.fori_loop(0, NB, last_layer, 0)

    def d_input(t, q):
        q = ops(q, cfg["pace"][2], NB)
        rows = pl.ds(pl.multiple_of(t * tt, tt), tt)
        dg = jnp.concatenate([S[pl.ds(pl.multiple_of(GB + j * 2 * T + t * tt, 16), tt), :] for j in range(NB)], axis=1)
        du = jnp.concatenate([S[pl.ds(pl.multiple_of(GB + j * 2 * T + T + t * tt, 16), tt), :] for j in range(NB)], axis=1)
        da = (mm(dg, wg[1], NT).astype(bf16).astype(f32) + mm(du, wu[1], NT).astype(bf16).astype(f32)).astype(bf16).astype(f32)
        wide = xh[rows, :].astype(f32)
        scale = rms_scale(wide)
        dot = jnp.sum(da * wide, -1, keepdims=True)
        dw = da * scale - wide * (scale * scale * scale * dot * (1.0 / D))
        dh[rows, :] = (dh[rows, :].astype(f32) + dw.astype(bf16).astype(f32)).astype(bf16)
        pltpu.make_async_copy(x_in.at[rows, :], xh.at[rows, :], x_sem).start()
        return q
    q = lax.fori_loop(0, T // tt, d_input, q)
    def renorm(t, q):
        rows = pl.ds(pl.multiple_of(t * tt, tt), tt)
        wide = xh[rows, :].astype(f32)
        a0 = (wide * rms_scale(wide)).astype(bf16)
        a[rows, :] = a0
        aT[:, rows] = a0.T
        return q
    pltpu.make_async_copy(x_in, xh, x_sem).wait()
    q = ops(q, 2, NB)
    lax.fori_loop(0, T // tt, renorm, 0)

    def first_layer(j, q):
        return block(0, j, 2 * GB, 2 * GB + T, NB + j, q, cfg["pace"][3], cfg["pace"][3])
    q = lax.fori_loop(0, NB, first_layer, q)
    if comm:
        lax.fori_loop(q, (LAST + 2) * n, op, 0)
        copies = [
            pltpu.make_async_remote_copy(
                src_ref=ss, dst_ref=squares.at[me], send_sem=sq_send.at[i], recv_sem=sq_recv.at[me],
                device_id={"dp": p}, device_id_type=pl.DeviceIdType.MESH)
            for i, p in enumerate(peers)]
        for c in copies:
            c.start()
        squares[me] = ss[...]
        for k in range(min(6, NB), NB):
            for d in range(2):
                onward(k, d).start()
        for r in range(LAST - RB + 2, LAST + 1):
            for s in range(n - 1):
                for b in range(NBLK):
                    if r - s == (2 * b if b < NB else 2 * b + gap if b <= ramp else b + ramp + gap):
                        for d in range(2):
                            hop(r, s, d).wait_send()
        for i, p in enumerate(peers):
            pltpu.make_async_remote_copy(
                src_ref=ss, dst_ref=squares.at[p], send_sem=sq_send.at[i], recv_sem=sq_recv.at[p],
                device_id={"dp": p}, device_id_type=pl.DeviceIdType.MESH).wait_recv()
        total = squares[0]
        for i in range(1, n):
            total = total + squares[i]
        total = jnp.sum(jnp.sum(total, axis=0, keepdims=True), axis=1, keepdims=True)
        factor[...] = jnp.broadcast_to(jnp.minimum(1.0, 0.5 * lax.rsqrt(total / float(NBLK * BR * BW) + 1e-30)), factor.shape)
        for c in copies:
            c.wait_send()
        for d in range(2):
            for k in range(NB):
                onward(k, d).wait_recv()
                onward(k, d).wait_send()
        for d in range(2):
            for b in range(NBLK):
                pltpu.make_async_copy(S.at[pl.ds(0, CH), :], (own00, own01, own10, own11)[2 * (b // NB) + d].at[b % NB], own_sem.at[d, b]).wait()
    else:
        cps = [pltpu.make_async_copy(S.at[pl.ds(b * BR + d * CH, CH), :], (own00, own01, own10, own11)[2 * (b // NB) + d].at[b % NB], own_sem.at[d, b]) for d in range(2) for b in range(NBLK)]
        for c in cps: c.start()
        for c in cps: c.wait()


def k1(x, dy, wg, wu, wd, n, tt=512, tb=512, comm=True, cid=0, pace=(5, 5, 6, 6), gap=0, quick=4):
    T, D = x.shape
    F = wg.shape[2]
    NB = F // BW
    NBLK = 2 * NB
    H = D // (2 * n); CH = 3 * H
    GB = NB * 3 * D
    cfg = dict(n=n, T=T, D=D, F=F, tt=min(tt, T), tb=min(tb, T), comm=comm, pace=pace, gap=gap, quick=quick)
    any_ = pl.BlockSpec(memory_space=pl.ANY)
    flops = 18 * 2 * T * D * F
    return pl.pallas_call(
        functools.partial(kernel, cfg),
        out_shape=(jax.ShapeDtypeStruct((NB, CH, BW), bf16),) * 6 + (jax.ShapeDtypeStruct((8, 128), f32),),
        in_specs=[any_] * 5,
        out_specs=(any_,) * 6 + (pl.BlockSpec(memory_space=pltpu.VMEM),),
        scratch_shapes=[
            pltpu.VMEM((max(GB + NB * 2 * T, 2 * GB + 2 * T), BW), bf16),
            pltpu.VMEM((T, D), bf16), pltpu.VMEM((T, D), bf16), pltpu.VMEM((D, T), bf16), pltpu.VMEM((T, D), bf16),
            pltpu.VMEM((T, BW), bf16),
            pltpu.VMEM((2, D, F), bf16), pltpu.VMEM((2, D, F), bf16), pltpu.VMEM((2, F, D), bf16),
            pltpu.VMEM((2, RB * (n - 1), CH, BW), bf16),
            pltpu.SemaphoreType.DMA((8,)), pltpu.SemaphoreType.DMA, pltpu.SemaphoreType.DMA((2, NBLK)),
            pltpu.SemaphoreType.DMA((2, RB * (n - 1))), pltpu.SemaphoreType.DMA((2, RB * (n - 1))), pltpu.SemaphoreType.REGULAR((2,)),
            pltpu.SemaphoreType.DMA((2, NB)), pltpu.SemaphoreType.DMA((2, NB)),
            pltpu.VMEM((8, 128), f32), pltpu.VMEM((n, 8, 128), f32), pltpu.SemaphoreType.DMA((n - 1,)), pltpu.SemaphoreType.DMA((n,)),
        ],
        compiler_params=pltpu.CompilerParams(vmem_limit_bytes=67043328, collective_id=cid if comm else None, has_side_effects=True),
        cost_estimate=pl.CostEstimate(flops=flops, bytes_accessed=40 * 10**6, transcendentals=0),
        name="grads")(x, dy, wg, wu, wd)


def adam_math(w, m, v, g):
    m = 0.9 * m + 0.1 * g
    v = 0.95 * v + 0.05 * g * g
    step = m * lax.rsqrt(v + 1e-8) + 0.1 * w
    return (w - 0.02 * step).astype(bf16), m, v


def adam_kernel(layers, idx_ref, fac_ref, *refs):
    k = len(layers)
    pays, ins, outs = refs[:k], refs[k : k + 9], refs[-17:-8]
    gbuf, wbuf, wdown, fbuf, fdown, gsem, isem, osem = refs[-8:]
    factor = fac_ref[0:1, 0:1]

    def place(i, a):
        which, kind = a // 3, a % 3
        if which == 0:
            return wdown.at[i] if kind == 2 else wbuf.at[i, kind]
        return fdown.at[i, which - 1] if kind == 2 else fbuf.at[i, which - 1, kind]

    def rows(arrays, i, a):
        return arrays[a].at[layers[i], :, idx_ref[i]] if a % 3 == 2 else arrays[a].at[layers[i], idx_ref[i]]

    loads = [[pltpu.make_async_copy(rows(ins, i, a), place(i, a), isem.at[i, a]) for a in range(9)] for i in range(k)]
    pay_loads = [pltpu.make_async_copy(pays[i], gbuf.at[i], gsem.at[i]) for i in range(k)]
    stores = [[pltpu.make_async_copy(place(i, a), rows(outs, i, a), osem.at[i, a]) for a in range(9)] for i in range(k)]
    for i in range(k):
        pay_loads[i].start()
        for kind in range(3):
            for a in range(kind, 9, 3):
                loads[i][a].start()
    hr = wdown.shape[2]
    for i in range(k):
        pay_loads[i].wait()
        def step(w, m, v, at, g):
            new = adam_math(w[at].astype(f32), m[at], v[at], g.astype(f32) * factor)
            for ref, value in zip((w, m, v), new, strict=True):
                ref[at] = value
        for kind in range(3):
            for a in range(kind, 9, 3):
                loads[i][a].wait()
            def block(j, _):
                if kind < 2:
                    cols = pl.ds(pl.multiple_of(j * BW, BW), BW)
                    step(wbuf.at[i, kind], fbuf.at[i, 0, kind], fbuf.at[i, 1, kind], (slice(None), cols), gbuf[i, j, kind])
                else:
                    for cg in range(wdown.shape[3] // BW):
                        at = (j, slice(None), slice(cg * BW, (cg + 1) * BW))
                        step(wdown.at[i], fdown.at[i, 0], fdown.at[i, 1], at, gbuf[i, j, 2, cg * hr : (cg + 1) * hr])
                return 0
            lax.fori_loop(0, gbuf.shape[1], block, 0)
            for a in range(kind, 9, 3):
                stores[i][a].start()
    for piece in stores:
        for c in piece:
            c.wait()


def adam_call(factor, pieces, ins, prev):
    k = len(pieces)
    layers = tuple(l for l, _, _ in pieces)
    idx = jnp.stack([c for _, c, _ in pieces]).astype(jnp.int32)
    pays = [g for _, _, g in pieces]
    hbm = pl.BlockSpec(memory_space=pl.ANY)
    kept = [] if prev is None else list(prev)
    size = k * pays[0].size
    rows, down = ins[0].shape[2:], (ins[2].shape[1],) + ins[2].shape[3:]
    return pl.pallas_call(
        functools.partial(adam_kernel, layers),
        grid_spec=pltpu.PrefetchScalarGridSpec(
            num_scalar_prefetch=1, grid=(1,),
            in_specs=[pl.BlockSpec((8, 128), lambda i, idx: (0, 0))] + [hbm] * (k + 9 + len(kept)),
            out_specs=[hbm] * 9,
            scratch_shapes=[
                pltpu.VMEM((k,) + pays[0].shape, bf16), pltpu.VMEM((k, 2) + rows, bf16), pltpu.VMEM((k,) + down, bf16),
                pltpu.VMEM((k, 2, 2) + rows, f32), pltpu.VMEM((k, 2) + down, f32),
                pltpu.SemaphoreType.DMA((k,)), pltpu.SemaphoreType.DMA((k, 9)), pltpu.SemaphoreType.DMA((k, 9))]),
        out_shape=[jax.ShapeDtypeStruct(x.shape, x.dtype) for x in ins],
        input_output_aliases={} if prev is None else {2 + k + 9 + i: i for i in range(9)},
        compiler_params=pltpu.CompilerParams(vmem_limit_bytes=62 * 2**20),
        cost_estimate=pl.CostEstimate(flops=10**9 * k, bytes_accessed=22 * size, transcendentals=size),
        name="adamw")(idx, factor, *pays, *ins, *kept)


def views(arrays, n):
    out = []
    for i, a in enumerate(arrays):
        L, r, c = a.shape
        out.append(a.reshape(L, 2 * n, r // (2 * n), c) if i % 3 < 2 else a.reshape(L, r // BW, 2 * n, BW // (2 * n), c))
    return out


def solution(mesh):
    n = mesh.shape["dp"]
    to = ([(i, (i + 1) % n) for i in range(n)], [(i, (i - 1) % n) for i in range(n)])

    def step(x, dy, *arrays):
        me = lax.axis_index("dp")
        *sums, factor = k1(x[0], dy[0], *arrays[:3], n)
        _, _, F = arrays[0].shape
        ins = views(arrays, n)
        last, first, came = ([o.reshape(F // BW, 3, o.shape[1] // 3, BW) for o in sums[i : i + 2]] for i in (0, 2, 4))

        def pieces(layer, pays, hops):
            return [(layer, 2 * lax.rem(me - hops + n, n), pays[0]), (layer, 2 * lax.rem(me + hops, n) + 1, pays[1])]

        waiting = pieces(1, last, 0) + pieces(0, first, 0) + pieces(1, came, 1)
        outs, last = None, came
        for s in range(1, n):
            ahead = []
            first = list(first)
            for d in range(2):
                first[d] = lax.ppermute(first[d], "dp", to[d])
            if s < n - 1:
                for d in range(2):
                    ahead.append(lax.ppermute(last[d], "dp", to[d]))
            outs = adam_call(factor, waiting, ins, outs)
            waiting = pieces(0, first, s) + (pieces(1, ahead, s + 1) if ahead else [])
            last = ahead
        outs = adam_call(factor, waiting, ins, outs)
        return tuple(o.reshape(w.shape) for o, w in zip(outs, arrays))

    step = jax.shard_map(
        step,
        mesh=mesh,
        in_specs=(P(("rep", "dp"), None, None),) * 2 + (P(None, None, None),) * 9,
        out_specs=(P("rep", None, None),) * 9,
        check_vma=False,
    )
    return step
```

```python
import functools

import jax
import jax.numpy as jnp
from jax import lax
from jax.experimental import pallas as pl
from jax.experimental.pallas import tpu as pltpu
from jax.sharding import PartitionSpec as P


BW = 256
RB = 3
f32, bf16 = jnp.float32, jnp.bfloat16
NT = (((1,), (1,)), ((), ()))
TN = (((0,), (0,)), ((), ()))


def mm(a, b, dims=(((1,), (0,)), ((), ()))):
    return lax.dot_general(a, b, dims, preferred_element_type=f32)


def rms_scale(wide):
    return lax.rsqrt(jnp.mean(wide * wide, -1, keepdims=True) + 1e-6)


def sigmoid(x):
    return 0.5 * jnp.tanh(0.5 * x) + 0.5


def kernel(cfg, x_in, dy_in, wg_in, wu_in, wd_in, own00, own01, own10, own11, got0, got1, factor, S, xh, a, aT, dh, hid, wg, wu, wd, recv,
           load_sem, block_sem, x_sem, own_sem, send_sem, recv_sem, credit, got_send, got_recv, ss, squares, sq_send, sq_recv):
    n, T, D, F, tt, tb, comm = cfg["n"], cfg["T"], cfg["D"], cfg["F"], cfg["tt"], cfg["tb"], cfg["comm"]
    NB = F // BW
    NBLK = 2 * NB
    H = D // (2 * n)
    CH = 3 * H
    BR = 3 * D
    GB = NB * BR
    hr = BW // (2 * n)
    ncg = D // BW
    ramp, gap = min(3, NB - 1), cfg["gap"]
    def start(b):
        return jnp.where(b <= ramp, 2 * b, jnp.where(b < NB, b + ramp, b + ramp + gap))
    LAST = NBLK - 1 + ramp + gap + n - 2
    ahead = ((LAST - 2, range(0, min(1, NB))), (LAST - 1, range(1, min(3, NB))), (LAST, range(3, min(6, NB))))
    me = lax.axis_index("dp")
    right, left = lax.rem(me + 1, n), lax.rem(me + n - 1, n)
    peers = [lax.rem(me + i, n) for i in range(1, n)]

    x_load = pltpu.make_async_copy(x_in, xh, load_sem.at[0])
    dy_load = pltpu.make_async_copy(dy_in, dh, load_sem.at[1])
    down_loads = [pltpu.make_async_copy(wd_in.at[l], wd.at[l], load_sem.at[2 + l]) for l in range(2)]
    last_loads = [pltpu.make_async_copy(s.at[1], d.at[1], load_sem.at[4 + i]) for i, (s, d) in enumerate(((wg_in, wg), (wu_in, wu)))]
    def block_loads(j):
        cols = pl.ds(pl.multiple_of(j * BW, BW), BW)
        return [pltpu.make_async_copy(s.at[0, :, cols], d.at[0, :, cols], block_sem.at[i, j]) for i, (s, d) in enumerate(((wg_in, wg), (wu_in, wu)))]
    x_load.start()
    if comm:
        barrier = pltpu.get_barrier_semaphore()
        for p in peers:
            pl.semaphore_signal(barrier, inc=1, device_id={"dp": p}, device_id_type=pl.DeviceIdType.MESH)
    ss[...] = jnp.zeros_like(ss)

    def chunk_row(b, c, d):
        return pl.multiple_of(b * BR + (2 * c + d) * CH, 16)

    def chunk_of(s, d):
        return lax.rem(me + 2 * n - 1 - s, n) if d == 0 else lax.rem(me + 1 + s, n)

    def block_of(r, s):
        z = r - s
        b = jnp.where(z <= 2 * ramp, lax.div(z, 2), jnp.where(z < NB + ramp, z - ramp, z - ramp - gap))
        live = ((z >= 0) & (z <= 2 * ramp) & (lax.rem(z, 2) == 0)) | ((z > 2 * ramp) & (z < NB + ramp)) | (z >= NB + ramp + gap)
        return b, live & (b < NBLK)

    def hop(r, s, d):
        b, _ = block_of(r, s)
        slot = lax.rem(r, RB) * (n - 1) + s
        return pltpu.make_async_remote_copy(
            src_ref=S.at[pl.ds(chunk_row(b, chunk_of(s, d), d), CH), :], dst_ref=recv.at[d, slot],
            send_sem=send_sem.at[d, slot], recv_sem=recv_sem.at[d, slot],
            device_id={"dp": right if d == 0 else left}, device_id_type=pl.DeviceIdType.MESH)

    def arrival(d, slot):
        return pltpu.make_async_remote_copy(
            src_ref=recv.at[d, slot], dst_ref=recv.at[d, slot], send_sem=send_sem.at[d, slot], recv_sem=recv_sem.at[d, slot],
            device_id={"dp": right if d == 0 else left}, device_id_type=pl.DeviceIdType.MESH)

    def onward(k, d):
        return pltpu.make_async_remote_copy(
            src_ref=S.at[pl.ds(chunk_row(k, me, d), CH), :], dst_ref=(got0, got1)[d].at[k],
            send_sem=got_send.at[d, k], recv_sem=got_recv.at[d, k],
            device_id={"dp": right if d == 0 else left}, device_id_type=pl.DeviceIdType.MESH)

    def op(q, _):
        r, s = lax.div(q, n), lax.rem(q, n)
        b, live = block_of(r, s)
        @pl.when((s == 0) & (r >= RB) & (r <= LAST))
        def _():
            pl.semaphore_wait(credit.at[0], 1)
            pl.semaphore_wait(credit.at[1], 1)
        @pl.when(live & (s >= 1))
        def _():
            slot = lax.rem(r + RB - 1, RB) * (n - 1) + s - 1
            for d in range(2):
                arrival(d, slot).wait_recv()
                rows = pl.ds(chunk_row(b, chunk_of(s, d), d), CH)
                total = (S[rows, :].astype(f32) + recv[d, slot].astype(f32)).astype(bf16)
                S[rows, :] = total
                @pl.when(s == n - 1)
                def _():
                    t = total.astype(f32)
                    t = t * t
                    ss[...] += functools.reduce(jnp.add, [t[i * 8:(i + 1) * 8, h * 128:(h + 1) * 128] for i in range(CH // 8) for h in range(BW // 128)])
        @pl.when(live & (s == n - 1))
        def _():
            for d in range(2):
                rows = pl.ds(chunk_row(b, me, d), CH)
                @pl.when(b < NB)
                def _():
                    pltpu.make_async_copy(S.at[rows, :], (own00, own01)[d].at[b], own_sem.at[d, b]).start()
                @pl.when(b >= NB)
                def _():
                    pltpu.make_async_copy(S.at[rows, :], (own10, own11)[d].at[b - NB], own_sem.at[d, b]).start()
        _, before = block_of(r - RB, s)
        @pl.when((s <= n - 2) & (r >= RB) & before)
        def _():
            for d in range(2):
                hop(r - RB, s, d).wait_send()
        @pl.when(live & (s <= n - 2))
        def _():
            for d in range(2):
                hop(r, s, d).start()
        for when, blocks in ahead:
            @pl.when((s == n - 1) & (r == when))
            def _():
                for k in blocks:
                    for d in range(2):
                        onward(k, d).start()
        @pl.when((s == n - 1) & (r >= 1) & (r <= LAST - RB + 1))
        def _():
            pl.semaphore_signal(credit.at[0], inc=1, device_id={"dp": left}, device_id_type=pl.DeviceIdType.MESH)
            pl.semaphore_signal(credit.at[1], inc=1, device_id={"dp": right}, device_id_type=pl.DeviceIdType.MESH)
        return 0

    def ops(q, count, ready):
        if not comm:
            return q
        limit = n * start(ready)
        end = jnp.where(q + count < limit, q + count, limit)
        lax.fori_loop(q, end, op, 0)
        return end

    x_load.wait()
    for j in range(NB):
        for c in block_loads(j):
            c.start()
    down_loads[0].start()
    def norm_x(t, _):
        rows = pl.ds(pl.multiple_of(t * tt, tt), tt)
        wide = xh[rows, :].astype(f32)
        a[rows, :] = (wide * rms_scale(wide)).astype(bf16)
        return 0
    lax.fori_loop(0, T // tt, norm_x, 0)
    def fwd(j, _):
        for c in block_loads(j):
            c.wait()
        cols = pl.ds(pl.multiple_of(j * BW, BW), BW)
        for t in range(T // tt):
            at = a[t * tt:(t + 1) * tt, :]
            g = mm(at, wg[0, :, cols])
            u = mm(at, wu[0, :, cols])
            S[pl.ds(pl.multiple_of(GB + j * T + t * tt, 16), tt), :] = (g * sigmoid(g) * u).astype(bf16)
        return 0
    lax.fori_loop(0, NB, fwd, 0)
    down_loads[0].wait()
    for c in last_loads + [dy_load, down_loads[1]]:
        c.start()
    def fwd_down(t, _):
        rows = pl.ds(pl.multiple_of(t * tt, tt), tt)
        hidden = jnp.concatenate([S[pl.ds(pl.multiple_of(GB + j * T + t * tt, 16), tt), :] for j in range(NB)], axis=1)
        h = (xh[rows, :].astype(f32) + mm(hidden, wd[0]).astype(bf16).astype(f32)).astype(bf16)
        xh[rows, :] = h
        hw = h.astype(f32)
        a1 = (hw * rms_scale(hw)).astype(bf16)
        a[rows, :] = a1
        aT[:, rows] = a1.T
        return 0
    lax.fori_loop(0, T // tt, fwd_down, 0, unroll=cfg["unroll"])

    def block(l, j, dg0, du0, b, q, pace, pace2):
        cols = pl.ds(pl.multiple_of(j * BW, BW), BW)
        q = ops(q, pace, b)
        def tokens(t, q):
            rows = pl.ds(pl.multiple_of(t * tb, tb), tb)
            at = a[rows, :]
            g = mm(at, wg[l, :, cols])
            u = mm(at, wu[l, :, cols])
            dhid = mm(dh[rows, :], wd[l, cols, :], NT).astype(bf16).astype(f32)
            sg = sigmoid(g)
            s = g * sg
            hid[rows, :] = (s * u).astype(bf16)
            S[pl.ds(pl.multiple_of(du0 + t * tb, 16), tb), :] = (dhid * s).astype(bf16)
            S[pl.ds(pl.multiple_of(dg0 + t * tb, 16), tb), :] = (dhid * u * (sg + s * (1.0 - sg))).astype(bf16)
            return q
        q = lax.fori_loop(0, T // tb, tokens, q, unroll=True)
        base = b * BR
        def gate_up(w, k):
            for e in range(2 * n):
                S[pl.ds(pl.multiple_of(base + e * CH + k * H, 16), H), :] = w[e * H:(e + 1) * H]
        def down(w):
            for e in range(2 * n):
                for cg in range(ncg):
                    S[pl.ds(pl.multiple_of(base + e * CH + 2 * H + cg * hr, 16), hr), :] = w[e * hr:(e + 1) * hr, cg * BW:(cg + 1) * BW]
        dgv = lambda: S[pl.ds(pl.multiple_of(dg0, 16), T), :]
        duv = lambda: S[pl.ds(pl.multiple_of(du0, 16), T), :]
        q = ops(q, pace2, b)
        w = mm(aT[...], jnp.concatenate([dgv(), duv()], axis=1)).astype(bf16)
        gate_up(w[:, :BW], 0)
        gate_up(w[:, BW:], 1)
        down(mm(hid[...], dh[...], TN).astype(bf16))
        return q

    for c in last_loads + [dy_load, down_loads[1]]:
        c.wait()
    if comm:
        pl.semaphore_wait(barrier, n - 1)

    def between(q):
        def d_input(t, q):
            q = ops(q, cfg["pace"][2], NB)
            rows = pl.ds(pl.multiple_of(t * tt, tt), tt)
            dg = jnp.concatenate([S[pl.ds(pl.multiple_of(GB + j * 2 * T + t * tt, 16), tt), :] for j in range(NB)], axis=1)
            du = jnp.concatenate([S[pl.ds(pl.multiple_of(GB + j * 2 * T + T + t * tt, 16), tt), :] for j in range(NB)], axis=1)
            da = (mm(dg, wg[1], NT).astype(bf16).astype(f32) + mm(du, wu[1], NT).astype(bf16).astype(f32)).astype(bf16).astype(f32)
            wide = xh[rows, :].astype(f32)
            scale = rms_scale(wide)
            dot = jnp.sum(da * wide, -1, keepdims=True)
            dw = da * scale - wide * (scale * scale * scale * dot * (1.0 / D))
            dh[rows, :] = (dh[rows, :].astype(f32) + dw.astype(bf16).astype(f32)).astype(bf16)
            pltpu.make_async_copy(x_in.at[rows, :], xh.at[rows, :], x_sem).start()
            return q
        q = lax.fori_loop(0, T // tt, d_input, q)
        def renorm(t, q):
            rows = pl.ds(pl.multiple_of(t * tt, tt), tt)
            wide = xh[rows, :].astype(f32)
            a0 = (wide * rms_scale(wide)).astype(bf16)
            a[rows, :] = a0
            aT[:, rows] = a0.T
            return q
        pltpu.make_async_copy(x_in, xh, x_sem).wait()
        q = ops(q, 2, NB)
        lax.fori_loop(0, T // tt, renorm, 0)
        return q

    def blocks(b, q):
        q = lax.cond(b == NB, between, lambda q: q, q)
        last = b < NB
        dg0 = jnp.where(last, GB + b * 2 * T, 2 * GB)
        pace = cfg["pace"]
        return block(jnp.where(last, 1, 0), jnp.where(last, b, b - NB), dg0, dg0 + T, b, q,
                     jnp.where(b <= 2, n, jnp.where(last, pace[0], pace[3])), jnp.where(b <= 2, n, jnp.where(last, pace[1], pace[3])))
    q = lax.fori_loop(0, NBLK, blocks, 0)
    if comm:
        lax.fori_loop(q, (LAST + 2) * n, op, 0)
        copies = [
            pltpu.make_async_remote_copy(
                src_ref=ss, dst_ref=squares.at[me], send_sem=sq_send.at[i], recv_sem=sq_recv.at[me],
                device_id={"dp": p}, device_id_type=pl.DeviceIdType.MESH)
            for i, p in enumerate(peers)]
        for c in copies:
            c.start()
        squares[me] = ss[...]
        for k in range(min(6, NB), NB):
            for d in range(2):
                onward(k, d).start()
        for r in range(LAST - RB + 2, LAST + 1):
            for s in range(n - 1):
                for b in range(NBLK):
                    if r - s == (2 * b if b <= ramp else b + ramp if b < NB else b + ramp + gap):
                        for d in range(2):
                            hop(r, s, d).wait_send()
        for i, p in enumerate(peers):
            pltpu.make_async_remote_copy(
                src_ref=ss, dst_ref=squares.at[p], send_sem=sq_send.at[i], recv_sem=sq_recv.at[p],
                device_id={"dp": p}, device_id_type=pl.DeviceIdType.MESH).wait_recv()
        total = squares[0]
        for i in range(1, n):
            total = total + squares[i]
        total = jnp.sum(jnp.sum(total, axis=0, keepdims=True), axis=1, keepdims=True)
        factor[...] = jnp.broadcast_to(jnp.minimum(1.0, 0.5 * lax.rsqrt(total / float(NBLK * BR * BW) + 1e-30)), factor.shape)
        for c in copies:
            c.wait_send()
        for d in range(2):
            for k in range(NB):
                onward(k, d).wait_recv()
                onward(k, d).wait_send()
        for d in range(2):
            for b in range(NBLK):
                pltpu.make_async_copy(S.at[pl.ds(0, CH), :], (own00, own01, own10, own11)[2 * (b // NB) + d].at[b % NB], own_sem.at[d, b]).wait()
    else:
        cps = [pltpu.make_async_copy(S.at[pl.ds(b * BR + d * CH, CH), :], (own00, own01, own10, own11)[2 * (b // NB) + d].at[b % NB], own_sem.at[d, b]) for d in range(2) for b in range(NBLK)]
        for c in cps: c.start()
        for c in cps: c.wait()


def k1(x, dy, wg, wu, wd, n, tt=512, tb=512, comm=True, cid=0, pace=(4, 5, 4, 6), gap=2, unroll=True):
    T, D = x.shape
    F = wg.shape[2]
    NB = F // BW
    NBLK = 2 * NB
    H = D // (2 * n); CH = 3 * H
    GB = NB * 3 * D
    cfg = dict(n=n, T=T, D=D, F=F, tt=min(tt, T), tb=min(tb, T), comm=comm, pace=pace, gap=gap, unroll=unroll)
    any_ = pl.BlockSpec(memory_space=pl.ANY)
    flops = 18 * 2 * T * D * F
    return pl.pallas_call(
        functools.partial(kernel, cfg),
        out_shape=(jax.ShapeDtypeStruct((NB, CH, BW), bf16),) * 6 + (jax.ShapeDtypeStruct((8, 128), f32),),
        in_specs=[any_] * 5,
        out_specs=(any_,) * 6 + (pl.BlockSpec(memory_space=pltpu.VMEM),),
        scratch_shapes=[
            pltpu.VMEM((max(GB + NB * 2 * T, 2 * GB + 2 * T), BW), bf16),
            pltpu.VMEM((T, D), bf16), pltpu.VMEM((T, D), bf16), pltpu.VMEM((D, T), bf16), pltpu.VMEM((T, D), bf16),
            pltpu.VMEM((T, BW), bf16),
            pltpu.VMEM((2, D, F), bf16), pltpu.VMEM((2, D, F), bf16), pltpu.VMEM((2, F, D), bf16),
            pltpu.VMEM((2, RB * (n - 1), CH, BW), bf16),
            pltpu.SemaphoreType.DMA((6,)), pltpu.SemaphoreType.DMA((2, NB)), pltpu.SemaphoreType.DMA, pltpu.SemaphoreType.DMA((2, NBLK)),
            pltpu.SemaphoreType.DMA((2, RB * (n - 1))), pltpu.SemaphoreType.DMA((2, RB * (n - 1))), pltpu.SemaphoreType.REGULAR((2,)),
            pltpu.SemaphoreType.DMA((2, NB)), pltpu.SemaphoreType.DMA((2, NB)),
            pltpu.VMEM((8, 128), f32), pltpu.VMEM((n, 8, 128), f32), pltpu.SemaphoreType.DMA((n - 1,)), pltpu.SemaphoreType.DMA((n,)),
        ],
        compiler_params=pltpu.CompilerParams(vmem_limit_bytes=67043328, collective_id=cid if comm else None, has_side_effects=True),
        cost_estimate=pl.CostEstimate(flops=flops, bytes_accessed=40 * 10**6, transcendentals=0),
        name="grads")(x, dy, wg, wu, wd)


def adam_math(w, m, v, g):
    m = 0.9 * m + 0.1 * g
    v = 0.95 * v + 0.05 * g * g
    step = m * lax.rsqrt(v + 1e-8) + 0.1 * w
    return (w - 0.02 * step).astype(bf16), m, v


def adam_kernel(layers, idx_ref, fac_ref, *refs):
    k = len(layers)
    pays, ins, outs = refs[:k], refs[k : k + 9], refs[-17:-8]
    gbuf, wbuf, wdown, fbuf, fdown, gsem, isem, osem = refs[-8:]
    factor = fac_ref[0:1, 0:1]

    def place(i, a):
        which, kind = a // 3, a % 3
        if which == 0:
            return wdown.at[i] if kind == 2 else wbuf.at[i, kind]
        return fdown.at[i, which - 1] if kind == 2 else fbuf.at[i, which - 1, kind]

    def rows(arrays, i, a):
        return arrays[a].at[layers[i], :, idx_ref[i]] if a % 3 == 2 else arrays[a].at[layers[i], idx_ref[i]]

    loads = [[pltpu.make_async_copy(rows(ins, i, a), place(i, a), isem.at[i, a]) for a in range(9)] for i in range(k)]
    pay_loads = [pltpu.make_async_copy(pays[i], gbuf.at[i], gsem.at[i]) for i in range(k)]
    stores = [[pltpu.make_async_copy(place(i, a), rows(outs, i, a), osem.at[i, a]) for a in range(9)] for i in range(k)]
    for i in range(k):
        pay_loads[i].start()
        for kind in range(3):
            for a in range(kind, 9, 3):
                loads[i][a].start()
    hr = wdown.shape[2]
    for i in range(k):
        pay_loads[i].wait()
        def step(w, m, v, at, g):
            new = adam_math(w[at].astype(f32), m[at], v[at], g.astype(f32) * factor)
            for ref, value in zip((w, m, v), new, strict=True):
                ref[at] = value
        for kind in range(3):
            for a in range(kind, 9, 3):
                loads[i][a].wait()
            def block(j, _):
                if kind < 2:
                    cols = pl.ds(pl.multiple_of(j * BW, BW), BW)
                    step(wbuf.at[i, kind], fbuf.at[i, 0, kind], fbuf.at[i, 1, kind], (slice(None), cols), gbuf[i, j, kind])
                else:
                    for cg in range(wdown.shape[3] // BW):
                        at = (j, slice(None), slice(cg * BW, (cg + 1) * BW))
                        step(wdown.at[i], fdown.at[i, 0], fdown.at[i, 1], at, gbuf[i, j, 2, cg * hr : (cg + 1) * hr])
                return 0
            lax.fori_loop(0, gbuf.shape[1], block, 0)
            for a in range(kind, 9, 3):
                stores[i][a].start()
    for piece in stores:
        for c in piece:
            c.wait()


def adam_call(factor, pieces, ins, prev):
    k = len(pieces)
    layers = tuple(l for l, _, _ in pieces)
    idx = jnp.stack([c for _, c, _ in pieces]).astype(jnp.int32)
    pays = [g for _, _, g in pieces]
    hbm = pl.BlockSpec(memory_space=pl.ANY)
    kept = [] if prev is None else list(prev)
    size = k * pays[0].size
    rows, down = ins[0].shape[2:], (ins[2].shape[1],) + ins[2].shape[3:]
    return pl.pallas_call(
        functools.partial(adam_kernel, layers),
        grid_spec=pltpu.PrefetchScalarGridSpec(
            num_scalar_prefetch=1, grid=(1,),
            in_specs=[pl.BlockSpec((8, 128), lambda i, idx: (0, 0))] + [hbm] * (k + 9 + len(kept)),
            out_specs=[hbm] * 9,
            scratch_shapes=[
                pltpu.VMEM((k,) + pays[0].shape, bf16), pltpu.VMEM((k, 2) + rows, bf16), pltpu.VMEM((k,) + down, bf16),
                pltpu.VMEM((k, 2, 2) + rows, f32), pltpu.VMEM((k, 2) + down, f32),
                pltpu.SemaphoreType.DMA((k,)), pltpu.SemaphoreType.DMA((k, 9)), pltpu.SemaphoreType.DMA((k, 9))]),
        out_shape=[jax.ShapeDtypeStruct(x.shape, x.dtype) for x in ins],
        input_output_aliases={} if prev is None else {2 + k + 9 + i: i for i in range(9)},
        compiler_params=pltpu.CompilerParams(vmem_limit_bytes=62 * 2**20),
        cost_estimate=pl.CostEstimate(flops=10**9 * k, bytes_accessed=22 * size, transcendentals=size),
        name="adamw")(idx, factor, *pays, *ins, *kept)


def views(arrays, n):
    out = []
    for i, a in enumerate(arrays):
        L, r, c = a.shape
        out.append(a.reshape(L, 2 * n, r // (2 * n), c) if i % 3 < 2 else a.reshape(L, r // BW, 2 * n, BW // (2 * n), c))
    return out


def solution(mesh):
    n = mesh.shape["dp"]
    to = ([(i, (i + 1) % n) for i in range(n)], [(i, (i - 1) % n) for i in range(n)])

    def step(x, dy, *arrays):
        me = lax.axis_index("dp")
        *sums, factor = k1(x[0], dy[0], *arrays[:3], n)
        _, _, F = arrays[0].shape
        ins = views(arrays, n)
        last, first, came = ([o.reshape(F // BW, 3, o.shape[1] // 3, BW) for o in sums[i : i + 2]] for i in (0, 2, 4))

        def pieces(layer, pays, hops):
            return [(layer, 2 * lax.rem(me - hops + n, n), pays[0]), (layer, 2 * lax.rem(me + hops, n) + 1, pays[1])]

        waiting = pieces(1, last, 0) + pieces(0, first, 0) + pieces(1, came, 1)
        outs, last = None, came
        for s in range(1, n):
            ahead = []
            first = list(first)
            for d in range(2):
                first[d] = lax.ppermute(first[d], "dp", to[d])
            if s < n - 1:
                for d in range(2):
                    ahead.append(lax.ppermute(last[d], "dp", to[d]))
            for part in [waiting] if s < n - 1 else [waiting[:2], waiting[2:]]:
                outs = adam_call(factor, part, ins, outs)
            waiting = pieces(0, first, s) + (pieces(1, ahead, s + 1) if ahead else [])
            last = ahead
        outs = adam_call(factor, waiting, ins, outs)
        return tuple(o.reshape(w.shape) for o, w in zip(outs, arrays))

    step = jax.shard_map(
        step,
        mesh=mesh,
        in_specs=(P(("rep", "dp"), None, None),) * 2 + (P(None, None, None),) * 9,
        out_specs=(P("rep", None, None),) * 9,
        check_vma=False,
    )
    return step
```

```python
import functools

import jax
import jax.numpy as jnp
from jax import lax
from jax.experimental import pallas as pl
from jax.experimental.pallas import tpu as pltpu
from jax.sharding import PartitionSpec as P


BW = 256
RB = 3
f32, bf16 = jnp.float32, jnp.bfloat16
NT = (((1,), (1,)), ((), ()))
TN = (((0,), (0,)), ((), ()))


def mm(a, b, dims=(((1,), (0,)), ((), ()))):
    return lax.dot_general(a, b, dims, preferred_element_type=f32)


def rms_scale(wide):
    return lax.rsqrt(jnp.mean(wide * wide, -1, keepdims=True) + 1e-6)


def sigmoid(x):
    return 0.5 * jnp.tanh(0.5 * x) + 0.5


def kernel(cfg, x_in, dy_in, wg_in, wu_in, wd_in, own00, own01, own10, own11, got0, got1, factor, S, xh, a, aT, dh, hid, wg, wu, wd, recv,
           load_sem, block_sem, x_sem, own_sem, send_sem, recv_sem, credit, got_send, got_recv, ss, squares, sq_send, sq_recv):
    n, T, D, F, tt, tb, comm = cfg["n"], cfg["T"], cfg["D"], cfg["F"], cfg["tt"], cfg["tb"], cfg["comm"]
    NB = F // BW
    NBLK = 2 * NB
    H = D // (2 * n)
    CH = 3 * H
    BR = 3 * D
    GB = NB * BR
    hr = BW // (2 * n)
    ncg = D // BW
    ramp, gap = min(3, NB - 1), cfg["gap"]
    def start(b):
        return jnp.where(b <= ramp, 2 * b, jnp.where(b < NB, b + ramp, b + ramp + gap))
    LAST = NBLK - 1 + ramp + gap + n - 2
    ahead = ((LAST - 2, range(0, min(1, NB))), (LAST - 1, range(1, min(3, NB))), (LAST, range(3, min(6, NB))))
    me = lax.axis_index("dp")
    right, left = lax.rem(me + 1, n), lax.rem(me + n - 1, n)
    peers = [lax.rem(me + i, n) for i in range(1, n)]

    x_load = pltpu.make_async_copy(x_in, xh, load_sem.at[0])
    dy_load = pltpu.make_async_copy(dy_in, dh, load_sem.at[1])
    down_loads = [pltpu.make_async_copy(wd_in.at[l], wd.at[l], load_sem.at[2 + l]) for l in range(2)]
    last_loads = [pltpu.make_async_copy(s.at[1], d.at[1], load_sem.at[4 + i]) for i, (s, d) in enumerate(((wg_in, wg), (wu_in, wu)))]
    def block_loads(j):
        cols = pl.ds(pl.multiple_of(j * BW, BW), BW)
        return [pltpu.make_async_copy(s.at[0, :, cols], d.at[0, :, cols], block_sem.at[i, j]) for i, (s, d) in enumerate(((wg_in, wg), (wu_in, wu)))]
    x_load.start()
    if comm:
        barrier = pltpu.get_barrier_semaphore()
        for p in peers:
            pl.semaphore_signal(barrier, inc=1, device_id={"dp": p}, device_id_type=pl.DeviceIdType.MESH)
    ss[...] = jnp.zeros_like(ss)

    def chunk_row(b, c, d):
        return pl.multiple_of(b * BR + (2 * c + d) * CH, 16)

    def chunk_of(s, d):
        return lax.rem(me + 2 * n - 1 - s, n) if d == 0 else lax.rem(me + 1 + s, n)

    def block_of(r, s):
        z = r - s
        b = jnp.where(z <= 2 * ramp, lax.div(z, 2), jnp.where(z < NB + ramp, z - ramp, z - ramp - gap))
        live = ((z >= 0) & (z <= 2 * ramp) & (lax.rem(z, 2) == 0)) | ((z > 2 * ramp) & (z < NB + ramp)) | (z >= NB + ramp + gap)
        return b, live & (b < NBLK)

    def hop(r, s, d):
        b, _ = block_of(r, s)
        slot = lax.rem(r, RB) * (n - 1) + s
        return pltpu.make_async_remote_copy(
            src_ref=S.at[pl.ds(chunk_row(b, chunk_of(s, d), d), CH), :], dst_ref=recv.at[d, slot],
            send_sem=send_sem.at[d, slot], recv_sem=recv_sem.at[d, slot],
            device_id={"dp": right if d == 0 else left}, device_id_type=pl.DeviceIdType.MESH)

    def arrival(d, slot):
        return pltpu.make_async_remote_copy(
            src_ref=recv.at[d, slot], dst_ref=recv.at[d, slot], send_sem=send_sem.at[d, slot], recv_sem=recv_sem.at[d, slot],
            device_id={"dp": right if d == 0 else left}, device_id_type=pl.DeviceIdType.MESH)

    def onward(k, d):
        return pltpu.make_async_remote_copy(
            src_ref=S.at[pl.ds(chunk_row(k, me, d), CH), :], dst_ref=(got0, got1)[d].at[k],
            send_sem=got_send.at[d, k], recv_sem=got_recv.at[d, k],
            device_id={"dp": right if d == 0 else left}, device_id_type=pl.DeviceIdType.MESH)

    def op(q, _):
        r, s = lax.div(q, n), lax.rem(q, n)
        b, live = block_of(r, s)
        @pl.when((s == 0) & (r >= RB) & (r <= LAST))
        def _():
            pl.semaphore_wait(credit.at[0], 1)
            pl.semaphore_wait(credit.at[1], 1)
        @pl.when(live & (s >= 1))
        def _():
            slot = lax.rem(r + RB - 1, RB) * (n - 1) + s - 1
            for d in range(2):
                arrival(d, slot).wait_recv()
                rows = pl.ds(chunk_row(b, chunk_of(s, d), d), CH)
                total = (S[rows, :].astype(f32) + recv[d, slot].astype(f32)).astype(bf16)
                S[rows, :] = total
                @pl.when(s == n - 1)
                def _():
                    t = total.astype(f32)
                    t = t * t
                    ss[...] += functools.reduce(jnp.add, [t[i * 8:(i + 1) * 8, h * 128:(h + 1) * 128] for i in range(CH // 8) for h in range(BW // 128)])
        @pl.when(live & (s == n - 1))
        def _():
            for d in range(2):
                rows = pl.ds(chunk_row(b, me, d), CH)
                @pl.when(b < NB)
                def _():
                    pltpu.make_async_copy(S.at[rows, :], (own00, own01)[d].at[b], own_sem.at[d, b]).start()
                @pl.when(b >= NB)
                def _():
                    pltpu.make_async_copy(S.at[rows, :], (own10, own11)[d].at[b - NB], own_sem.at[d, b]).start()
        _, before = block_of(r - RB, s)
        @pl.when((s <= n - 2) & (r >= RB) & before)
        def _():
            for d in range(2):
                hop(r - RB, s, d).wait_send()
        @pl.when(live & (s <= n - 2))
        def _():
            for d in range(2):
                hop(r, s, d).start()
        for when, blocks in ahead:
            @pl.when((s == n - 1) & (r == when))
            def _():
                for k in blocks:
                    for d in range(2):
                        onward(k, d).start()
        @pl.when((s == n - 1) & (r >= 1) & (r <= LAST - RB + 1))
        def _():
            pl.semaphore_signal(credit.at[0], inc=1, device_id={"dp": left}, device_id_type=pl.DeviceIdType.MESH)
            pl.semaphore_signal(credit.at[1], inc=1, device_id={"dp": right}, device_id_type=pl.DeviceIdType.MESH)
        return 0

    def ops(q, count, ready):
        if not comm:
            return q
        limit = n * start(ready)
        end = jnp.where(q + count < limit, q + count, limit)
        lax.fori_loop(q, end, op, 0)
        return end

    x_load.wait()
    for j in range(NB):
        for c in block_loads(j):
            c.start()
    down_loads[0].start()
    def norm_x(t, _):
        rows = pl.ds(pl.multiple_of(t * tt, tt), tt)
        wide = xh[rows, :].astype(f32)
        a[rows, :] = (wide * rms_scale(wide)).astype(bf16)
        return 0
    lax.fori_loop(0, T // tt, norm_x, 0)
    def fwd(j, _):
        for c in block_loads(j):
            c.wait()
        cols = pl.ds(pl.multiple_of(j * BW, BW), BW)
        for t in range(T // tt):
            at = a[t * tt:(t + 1) * tt, :]
            g = mm(at, wg[0, :, cols])
            u = mm(at, wu[0, :, cols])
            S[pl.ds(pl.multiple_of(GB + j * T + t * tt, 16), tt), :] = (g * sigmoid(g) * u).astype(bf16)
        return 0
    lax.fori_loop(0, NB, fwd, 0)
    down_loads[0].wait()
    for c in last_loads + [dy_load, down_loads[1]]:
        c.start()
    def fwd_down(t, _):
        rows = pl.ds(pl.multiple_of(t * tt, tt), tt)
        hidden = jnp.concatenate([S[pl.ds(pl.multiple_of(GB + j * T + t * tt, 16), tt), :] for j in range(NB)], axis=1)
        h = (xh[rows, :].astype(f32) + mm(hidden, wd[0]).astype(bf16).astype(f32)).astype(bf16)
        xh[rows, :] = h
        hw = h.astype(f32)
        a1 = (hw * rms_scale(hw)).astype(bf16)
        a[rows, :] = a1
        aT[:, rows] = a1.T
        return 0
    lax.fori_loop(0, T // tt, fwd_down, 0, unroll=cfg["unroll"])

    def block(l, j, dg0, du0, b, q, pace, pace2):
        cols = pl.ds(pl.multiple_of(j * BW, BW), BW)
        q = ops(q, pace, b)
        def tokens(t, q):
            rows = pl.ds(pl.multiple_of(t * tb, tb), tb)
            at = a[rows, :]
            g = mm(at, wg[l, :, cols])
            u = mm(at, wu[l, :, cols])
            dhid = mm(dh[rows, :], wd[l, cols, :], NT).astype(bf16).astype(f32)
            sg = sigmoid(g)
            s = g * sg
            hid[rows, :] = (s * u).astype(bf16)
            S[pl.ds(pl.multiple_of(du0 + t * tb, 16), tb), :] = (dhid * s).astype(bf16)
            S[pl.ds(pl.multiple_of(dg0 + t * tb, 16), tb), :] = (dhid * u * (sg + s * (1.0 - sg))).astype(bf16)
            return q
        q = lax.fori_loop(0, T // tb, tokens, q, unroll=True)
        base = b * BR
        def gate_up(w, k):
            for e in range(2 * n):
                S[pl.ds(pl.multiple_of(base + e * CH + k * H, 16), H), :] = w[e * H:(e + 1) * H]
        def down(w):
            for e in range(2 * n):
                for cg in range(ncg):
                    S[pl.ds(pl.multiple_of(base + e * CH + 2 * H + cg * hr, 16), hr), :] = w[e * hr:(e + 1) * hr, cg * BW:(cg + 1) * BW]
        dgv = lambda: S[pl.ds(pl.multiple_of(dg0, 16), T), :]
        duv = lambda: S[pl.ds(pl.multiple_of(du0, 16), T), :]
        q = ops(q, pace2, b)
        w = mm(aT[...], jnp.concatenate([dgv(), duv()], axis=1)).astype(bf16)
        gate_up(w[:, :BW], 0)
        gate_up(w[:, BW:], 1)
        down(mm(hid[...], dh[...], TN).astype(bf16))
        return q

    for c in last_loads + [dy_load, down_loads[1]]:
        c.wait()
    if comm:
        pl.semaphore_wait(barrier, n - 1)

    def between(q):
        def d_input(t, q):
            q = ops(q, cfg["pace"][2], NB)
            rows = pl.ds(pl.multiple_of(t * tt, tt), tt)
            dg = jnp.concatenate([S[pl.ds(pl.multiple_of(GB + j * 2 * T + t * tt, 16), tt), :] for j in range(NB)], axis=1)
            du = jnp.concatenate([S[pl.ds(pl.multiple_of(GB + j * 2 * T + T + t * tt, 16), tt), :] for j in range(NB)], axis=1)
            da = (mm(dg, wg[1], NT).astype(bf16).astype(f32) + mm(du, wu[1], NT).astype(bf16).astype(f32)).astype(bf16).astype(f32)
            wide = xh[rows, :].astype(f32)
            scale = rms_scale(wide)
            dot = jnp.sum(da * wide, -1, keepdims=True)
            dw = da * scale - wide * (scale * scale * scale * dot * (1.0 / D))
            dh[rows, :] = (dh[rows, :].astype(f32) + dw.astype(bf16).astype(f32)).astype(bf16)
            pltpu.make_async_copy(x_in.at[rows, :], xh.at[rows, :], x_sem).start()
            return q
        q = lax.fori_loop(0, T // tt, d_input, q)
        def renorm(t, q):
            rows = pl.ds(pl.multiple_of(t * tt, tt), tt)
            wide = xh[rows, :].astype(f32)
            a0 = (wide * rms_scale(wide)).astype(bf16)
            a[rows, :] = a0
            aT[:, rows] = a0.T
            return q
        pltpu.make_async_copy(x_in, xh, x_sem).wait()
        q = ops(q, 2, NB)
        lax.fori_loop(0, T // tt, renorm, 0)
        return q

    def blocks(b, q):
        q = lax.cond(b == NB, between, lambda q: q, q)
        last = b < NB
        dg0 = jnp.where(last, GB + b * 2 * T, 2 * GB)
        pace = cfg["pace"]
        return block(jnp.where(last, 1, 0), jnp.where(last, b, b - NB), dg0, dg0 + T, b, q,
                     jnp.where(b <= 2, n, jnp.where(last, pace[0], pace[3])), jnp.where(b <= 2, n, jnp.where(last, pace[1], pace[3])))
    q = lax.fori_loop(0, NBLK, blocks, 0)
    if comm:
        lax.fori_loop(q, (LAST + 2) * n, op, 0)
        copies = [
            pltpu.make_async_remote_copy(
                src_ref=ss, dst_ref=squares.at[me], send_sem=sq_send.at[i], recv_sem=sq_recv.at[me],
                device_id={"dp": p}, device_id_type=pl.DeviceIdType.MESH)
            for i, p in enumerate(peers)]
        for c in copies:
            c.start()
        squares[me] = ss[...]
        for k in range(min(6, NB), NB):
            for d in range(2):
                onward(k, d).start()
        for r in range(LAST - RB + 2, LAST + 1):
            for s in range(n - 1):
                for b in range(NBLK):
                    if r - s == (2 * b if b <= ramp else b + ramp if b < NB else b + ramp + gap):
                        for d in range(2):
                            hop(r, s, d).wait_send()
        for i, p in enumerate(peers):
            pltpu.make_async_remote_copy(
                src_ref=ss, dst_ref=squares.at[p], send_sem=sq_send.at[i], recv_sem=sq_recv.at[p],
                device_id={"dp": p}, device_id_type=pl.DeviceIdType.MESH).wait_recv()
        total = squares[0]
        for i in range(1, n):
            total = total + squares[i]
        total = jnp.sum(jnp.sum(total, axis=0, keepdims=True), axis=1, keepdims=True)
        factor[...] = jnp.broadcast_to(jnp.minimum(1.0, 0.5 * lax.rsqrt(total / float(NBLK * BR * BW) + 1e-30)), factor.shape)
        for c in copies:
            c.wait_send()
        for d in range(2):
            for k in range(NB):
                onward(k, d).wait_recv()
                onward(k, d).wait_send()
        for d in range(2):
            for b in range(NBLK):
                pltpu.make_async_copy(S.at[pl.ds(0, CH), :], (own00, own01, own10, own11)[2 * (b // NB) + d].at[b % NB], own_sem.at[d, b]).wait()
    else:
        cps = [pltpu.make_async_copy(S.at[pl.ds(b * BR + d * CH, CH), :], (own00, own01, own10, own11)[2 * (b // NB) + d].at[b % NB], own_sem.at[d, b]) for d in range(2) for b in range(NBLK)]
        for c in cps: c.start()
        for c in cps: c.wait()


def k1(x, dy, wg, wu, wd, n, tt=512, tb=512, comm=True, cid=0, pace=(4, 5, 4, 6), gap=2, unroll=True):
    T, D = x.shape
    F = wg.shape[2]
    NB = F // BW
    NBLK = 2 * NB
    H = D // (2 * n); CH = 3 * H
    GB = NB * 3 * D
    cfg = dict(n=n, T=T, D=D, F=F, tt=min(tt, T), tb=min(tb, T), comm=comm, pace=pace, gap=gap, unroll=unroll)
    any_ = pl.BlockSpec(memory_space=pl.ANY)
    flops = 18 * 2 * T * D * F
    return pl.pallas_call(
        functools.partial(kernel, cfg),
        out_shape=(jax.ShapeDtypeStruct((NB, CH, BW), bf16),) * 6 + (jax.ShapeDtypeStruct((8, 128), f32),),
        in_specs=[any_] * 5,
        out_specs=(any_,) * 6 + (pl.BlockSpec(memory_space=pltpu.VMEM),),
        scratch_shapes=[
            pltpu.VMEM((max(GB + NB * 2 * T, 2 * GB + 2 * T), BW), bf16),
            pltpu.VMEM((T, D), bf16), pltpu.VMEM((T, D), bf16), pltpu.VMEM((D, T), bf16), pltpu.VMEM((T, D), bf16),
            pltpu.VMEM((T, BW), bf16),
            pltpu.VMEM((2, D, F), bf16), pltpu.VMEM((2, D, F), bf16), pltpu.VMEM((2, F, D), bf16),
            pltpu.VMEM((2, RB * (n - 1), CH, BW), bf16),
            pltpu.SemaphoreType.DMA((6,)), pltpu.SemaphoreType.DMA((2, NB)), pltpu.SemaphoreType.DMA, pltpu.SemaphoreType.DMA((2, NBLK)),
            pltpu.SemaphoreType.DMA((2, RB * (n - 1))), pltpu.SemaphoreType.DMA((2, RB * (n - 1))), pltpu.SemaphoreType.REGULAR((2,)),
            pltpu.SemaphoreType.DMA((2, NB)), pltpu.SemaphoreType.DMA((2, NB)),
            pltpu.VMEM((8, 128), f32), pltpu.VMEM((n, 8, 128), f32), pltpu.SemaphoreType.DMA((n - 1,)), pltpu.SemaphoreType.DMA((n,)),
        ],
        compiler_params=pltpu.CompilerParams(vmem_limit_bytes=67043328, collective_id=cid if comm else None, has_side_effects=True),
        cost_estimate=pl.CostEstimate(flops=flops, bytes_accessed=40 * 10**6, transcendentals=0),
        name="grads")(x, dy, wg, wu, wd)


def adam_math(w, m, v, g):
    m = 0.9 * m + 0.1 * g
    v = 0.95 * v + 0.05 * g * g
    step = m * lax.rsqrt(v + 1e-8) + 0.1 * w
    return (w - 0.02 * step).astype(bf16), m, v


def adam_kernel(n, where, fac_hbm, *refs):
    k = len(where)
    pays, ins, outs = refs[:k], refs[k : k + 9], refs[-19:-10]
    fac, gbuf, wbuf, wdown, fbuf, fdown, fsem, gsem, isem, osem = refs[-10:]
    me = lax.axis_index("dp")
    layers = [layer for layer, _, _ in where]
    chunks = [2 * lax.rem(me + (n - hops if d == 0 else hops), n) + d for _, d, hops in where]
    fac_load = pltpu.make_async_copy(fac_hbm, fac, fsem)

    def place(i, a):
        which, kind = a // 3, a % 3
        if which == 0:
            return wdown.at[i] if kind == 2 else wbuf.at[i, kind]
        return fdown.at[i, which - 1] if kind == 2 else fbuf.at[i, which - 1, kind]

    def rows(arrays, i, a):
        return arrays[a].at[layers[i], :, chunks[i]] if a % 3 == 2 else arrays[a].at[layers[i], chunks[i]]

    loads = [[pltpu.make_async_copy(rows(ins, i, a), place(i, a), isem.at[i, a]) for a in range(9)] for i in range(k)]
    pay_loads = [pltpu.make_async_copy(pays[i], gbuf.at[i], gsem.at[i]) for i in range(k)]
    stores = [[pltpu.make_async_copy(place(i, a), rows(outs, i, a), osem.at[i, a]) for a in range(9)] for i in range(k)]
    for i in range(k):
        pay_loads[i].start()
        for kind in range(3):
            for a in range(kind, 9, 3):
                loads[i][a].start()
        if i == 0:
            fac_load.start()
    hr = wdown.shape[2]
    fac_load.wait()
    factor = fac[0:1, 0:1]
    for i in range(k):
        pay_loads[i].wait()
        def step(w, m, v, at, g):
            new = adam_math(w[at].astype(f32), m[at], v[at], g.astype(f32) * factor)
            for ref, value in zip((w, m, v), new, strict=True):
                ref[at] = value
        for kind in range(3):
            for a in range(kind, 9, 3):
                loads[i][a].wait()
            def block(j, _):
                if kind < 2:
                    cols = pl.ds(pl.multiple_of(j * BW, BW), BW)
                    step(wbuf.at[i, kind], fbuf.at[i, 0, kind], fbuf.at[i, 1, kind], (slice(None), cols), gbuf[i, j, kind])
                else:
                    for cg in range(wdown.shape[3] // BW):
                        at = (j, slice(None), slice(cg * BW, (cg + 1) * BW))
                        step(wdown.at[i], fdown.at[i, 0], fdown.at[i, 1], at, gbuf[i, j, 2, cg * hr : (cg + 1) * hr])
                return 0
            lax.fori_loop(0, gbuf.shape[1], block, 0)
            for a in range(kind, 9, 3):
                stores[i][a].start()
    for piece in stores:
        for c in piece:
            c.wait()


def adam_call(n, factor, pieces, ins, prev):
    k = len(pieces)
    pays = [g for _, g in pieces]
    hbm = pl.BlockSpec(memory_space=pltpu.HBM)
    kept = [] if prev is None else list(prev)
    size = k * pays[0].size
    rows, down = ins[0].shape[2:], (ins[2].shape[1],) + ins[2].shape[3:]
    return pl.pallas_call(
        functools.partial(adam_kernel, n, tuple(w for w, _ in pieces)),
        in_specs=[hbm] * (1 + k + 9 + len(kept)),
        out_specs=[hbm] * 9,
        scratch_shapes=[
            pltpu.VMEM(factor.shape, f32),
            pltpu.VMEM((k,) + pays[0].shape, bf16), pltpu.VMEM((k, 2) + rows, bf16), pltpu.VMEM((k,) + down, bf16),
            pltpu.VMEM((k, 2, 2) + rows, f32), pltpu.VMEM((k, 2) + down, f32),
            pltpu.SemaphoreType.DMA, pltpu.SemaphoreType.DMA((k,)), pltpu.SemaphoreType.DMA((k, 9)), pltpu.SemaphoreType.DMA((k, 9))],
        out_shape=[jax.ShapeDtypeStruct(x.shape, x.dtype) for x in ins],
        input_output_aliases={} if prev is None else {1 + k + 9 + i: i for i in range(9)},
        compiler_params=pltpu.CompilerParams(vmem_limit_bytes=62 * 2**20),
        cost_estimate=pl.CostEstimate(flops=10**9 * k, bytes_accessed=22 * size, transcendentals=size),
        name="adamw")(factor, *pays, *ins, *kept)


def views(arrays, n):
    out = []
    for i, a in enumerate(arrays):
        L, r, c = a.shape
        out.append(a.reshape(L, 2 * n, r // (2 * n), c) if i % 3 < 2 else a.reshape(L, r // BW, 2 * n, BW // (2 * n), c))
    return out


def solution(mesh):
    n = mesh.shape["dp"]
    to = ([(i, (i + 1) % n) for i in range(n)], [(i, (i - 1) % n) for i in range(n)])

    def step(x, dy, *arrays):
        *sums, factor = k1(x[0], dy[0], *arrays[:3], n)
        _, _, F = arrays[0].shape
        ins = views(arrays, n)
        last, first, came = ([o.reshape(F // BW, 3, o.shape[1] // 3, BW) for o in sums[i : i + 2]] for i in (0, 2, 4))

        def pieces(layer, pays, hops):
            return [((layer, d, hops), pays[d]) for d in range(2)]

        waiting = pieces(1, last, 0) + pieces(0, first, 0) + pieces(1, came, 1)
        outs, last = None, came
        for s in range(1, n):
            ahead = []
            first = list(first)
            for d in range(2):
                first[d] = lax.ppermute(first[d], "dp", to[d])
            if s < n - 1:
                for d in range(2):
                    ahead.append(lax.ppermute(last[d], "dp", to[d]))
            for part in [waiting] if s < n - 1 else [waiting[:2], waiting[2:]]:
                outs = adam_call(n, factor, part, ins, outs)
            waiting = pieces(0, first, s) + (pieces(1, ahead, s + 1) if ahead else [])
            last = ahead
        outs = adam_call(n, factor, waiting, ins, outs)
        return tuple(o.reshape(w.shape) for o, w in zip(outs, arrays))

    step = jax.shard_map(
        step,
        mesh=mesh,
        in_specs=(P(("rep", "dp"), None, None),) * 2 + (P(None, None, None),) * 9,
        out_specs=(P("rep", None, None),) * 9,
        check_vma=False,
    )
    return step
```

```python
import functools

import jax
import jax.numpy as jnp
from jax import lax
from jax.experimental import pallas as pl
from jax.experimental.pallas import tpu as pltpu
from jax.sharding import PartitionSpec as P


BW = 256
RB = 3
f32, bf16 = jnp.float32, jnp.bfloat16
NT = (((1,), (1,)), ((), ()))
TN = (((0,), (0,)), ((), ()))


def mm(a, b, dims=(((1,), (0,)), ((), ()))):
    return lax.dot_general(a, b, dims, preferred_element_type=f32)


def rms_scale(wide):
    return lax.rsqrt(jnp.mean(wide * wide, -1, keepdims=True) + 1e-6)


def sigmoid(x):
    return 0.5 * jnp.tanh(0.5 * x) + 0.5


def kernel(cfg, x_in, dy_in, wg_in, wu_in, wd_in, own00, own01, own10, own11, got0, got1, factor, S, xh, a, aT, dh, hid, wg, wu, wd, recv,
           load_sem, block_sem, x_sem, own_sem, send_sem, recv_sem, credit, got_send, got_recv, ss, squares, sq_send, sq_recv):
    n, T, D, F, tt, tb, comm = cfg["n"], cfg["T"], cfg["D"], cfg["F"], cfg["tt"], cfg["tb"], cfg["comm"]
    NB = F // BW
    NBLK = 2 * NB
    H = D // (2 * n)
    CH = 3 * H
    BR = 3 * D
    GB = NB * BR
    hr = BW // (2 * n)
    ncg = D // BW
    ramp, gap = min(3, NB - 1), cfg["gap"]
    def start(b):
        return jnp.where(b <= ramp, 2 * b, jnp.where(b < NB, b + ramp, b + ramp + gap))
    LAST = NBLK - 1 + ramp + gap + n - 2
    ahead = ((LAST - 2, range(0, min(1, NB))), (LAST - 1, range(1, min(3, NB))), (LAST, range(3, min(6, NB))))
    me = lax.axis_index("dp")
    right, left = lax.rem(me + 1, n), lax.rem(me + n - 1, n)
    peers = [lax.rem(me + i, n) for i in range(1, n)]

    x_load = pltpu.make_async_copy(x_in, xh, load_sem.at[0])
    dy_load = pltpu.make_async_copy(dy_in, dh, load_sem.at[1])
    down_loads = [pltpu.make_async_copy(wd_in.at[l], wd.at[l], load_sem.at[2 + l]) for l in range(2)]
    last_loads = [pltpu.make_async_copy(s.at[1], d.at[1], load_sem.at[4 + i]) for i, (s, d) in enumerate(((wg_in, wg), (wu_in, wu)))]
    def block_loads(j):
        cols = pl.ds(pl.multiple_of(j * BW, BW), BW)
        return [pltpu.make_async_copy(s.at[0, :, cols], d.at[0, :, cols], block_sem.at[i, j]) for i, (s, d) in enumerate(((wg_in, wg), (wu_in, wu)))]
    x_load.start()
    if comm:
        barrier = pltpu.get_barrier_semaphore()
        for p in peers:
            pl.semaphore_signal(barrier, inc=1, device_id={"dp": p}, device_id_type=pl.DeviceIdType.MESH)
    ss[...] = jnp.zeros_like(ss)

    def chunk_row(b, c, d):
        return pl.multiple_of(b * BR + (2 * c + d) * CH, 16)

    def chunk_of(s, d):
        return lax.rem(me + 2 * n - 1 - s, n) if d == 0 else lax.rem(me + 1 + s, n)

    def block_of(r, s):
        z = r - s
        b = jnp.where(z <= 2 * ramp, lax.div(z, 2), jnp.where(z < NB + ramp, z - ramp, z - ramp - gap))
        live = ((z >= 0) & (z <= 2 * ramp) & (lax.rem(z, 2) == 0)) | ((z > 2 * ramp) & (z < NB + ramp)) | (z >= NB + ramp + gap)
        return b, live & (b < NBLK)

    def hop(r, s, d):
        b, _ = block_of(r, s)
        slot = lax.rem(r, RB) * (n - 1) + s
        return pltpu.make_async_remote_copy(
            src_ref=S.at[pl.ds(chunk_row(b, chunk_of(s, d), d), CH), :], dst_ref=recv.at[d, slot],
            send_sem=send_sem.at[d, slot], recv_sem=recv_sem.at[d, slot],
            device_id={"dp": right if d == 0 else left}, device_id_type=pl.DeviceIdType.MESH)

    def arrival(d, slot):
        return pltpu.make_async_remote_copy(
            src_ref=recv.at[d, slot], dst_ref=recv.at[d, slot], send_sem=send_sem.at[d, slot], recv_sem=recv_sem.at[d, slot],
            device_id={"dp": right if d == 0 else left}, device_id_type=pl.DeviceIdType.MESH)

    def onward(k, d):
        return pltpu.make_async_remote_copy(
            src_ref=S.at[pl.ds(chunk_row(k, me, d), CH), :], dst_ref=(got0, got1)[d].at[k],
            send_sem=got_send.at[d, k], recv_sem=got_recv.at[d, k],
            device_id={"dp": right if d == 0 else left}, device_id_type=pl.DeviceIdType.MESH)

    def op(q, _):
        r, s = lax.div(q, n), lax.rem(q, n)
        b, live = block_of(r, s)
        @pl.when((s == 0) & (r >= RB) & (r <= LAST))
        def _():
            pl.semaphore_wait(credit.at[0], 1)
            pl.semaphore_wait(credit.at[1], 1)
        @pl.when(live & (s >= 1))
        def _():
            slot = lax.rem(r + RB - 1, RB) * (n - 1) + s - 1
            for d in range(2):
                arrival(d, slot).wait_recv()
                rows = pl.ds(chunk_row(b, chunk_of(s, d), d), CH)
                total = (S[rows, :].astype(f32) + recv[d, slot].astype(f32)).astype(bf16)
                S[rows, :] = total
                @pl.when(s == n - 1)
                def _():
                    t = total.astype(f32)
                    t = t * t
                    ss[...] += functools.reduce(jnp.add, [t[i * 8:(i + 1) * 8, h * 128:(h + 1) * 128] for i in range(CH // 8) for h in range(BW // 128)])
        @pl.when(live & (s == n - 1))
        def _():
            for d in range(2):
                rows = pl.ds(chunk_row(b, me, d), CH)
                @pl.when(b < NB)
                def _():
                    pltpu.make_async_copy(S.at[rows, :], (own00, own01)[d].at[b], own_sem.at[d, b]).start()
                @pl.when(b >= NB)
                def _():
                    pltpu.make_async_copy(S.at[rows, :], (own10, own11)[d].at[b - NB], own_sem.at[d, b]).start()
        _, before = block_of(r - RB, s)
        @pl.when((s <= n - 2) & (r >= RB) & before)
        def _():
            for d in range(2):
                hop(r - RB, s, d).wait_send()
        @pl.when(live & (s <= n - 2))
        def _():
            for d in range(2):
                hop(r, s, d).start()
        for when, blocks in ahead:
            @pl.when((s == n - 1) & (r == when))
            def _():
                for k in blocks:
                    for d in range(2):
                        onward(k, d).start()
        @pl.when((s == n - 1) & (r >= 1) & (r <= LAST - RB + 1))
        def _():
            pl.semaphore_signal(credit.at[0], inc=1, device_id={"dp": left}, device_id_type=pl.DeviceIdType.MESH)
            pl.semaphore_signal(credit.at[1], inc=1, device_id={"dp": right}, device_id_type=pl.DeviceIdType.MESH)
        return 0

    def ops(q, count, ready):
        if not comm:
            return q
        limit = n * start(ready)
        end = jnp.where(q + count < limit, q + count, limit)
        lax.fori_loop(q, end, op, 0)
        return end

    x_load.wait()
    for j in range(NB):
        for c in block_loads(j):
            c.start()
    down_loads[0].start()
    def norm_x(t, _):
        rows = pl.ds(pl.multiple_of(t * tt, tt), tt)
        wide = xh[rows, :].astype(f32)
        a[rows, :] = (wide * rms_scale(wide)).astype(bf16)
        return 0
    lax.fori_loop(0, T // tt, norm_x, 0)
    def fwd(j, _):
        for c in block_loads(j):
            c.wait()
        cols = pl.ds(pl.multiple_of(j * BW, BW), BW)
        for t in range(T // tt):
            at = a[t * tt:(t + 1) * tt, :]
            g = mm(at, wg[0, :, cols])
            u = mm(at, wu[0, :, cols])
            S[pl.ds(pl.multiple_of(GB + j * T + t * tt, 16), tt), :] = (g * sigmoid(g) * u).astype(bf16)
        return 0
    lax.fori_loop(0, NB, fwd, 0)
    down_loads[0].wait()
    for c in last_loads + [dy_load, down_loads[1]]:
        c.start()
    def fwd_down(t, _):
        rows = pl.ds(pl.multiple_of(t * tt, tt), tt)
        hidden = jnp.concatenate([S[pl.ds(pl.multiple_of(GB + j * T + t * tt, 16), tt), :] for j in range(NB)], axis=1)
        h = (xh[rows, :].astype(f32) + mm(hidden, wd[0]).astype(bf16).astype(f32)).astype(bf16)
        xh[rows, :] = h
        hw = h.astype(f32)
        a1 = (hw * rms_scale(hw)).astype(bf16)
        a[rows, :] = a1
        aT[:, rows] = a1.T
        return 0
    lax.fori_loop(0, T // tt, fwd_down, 0, unroll=cfg["unroll"])

    def block(l, j, dg0, du0, b, q, pace, pace2):
        cols = pl.ds(pl.multiple_of(j * BW, BW), BW)
        q = ops(q, pace, b)
        def tokens(t, q):
            rows = pl.ds(pl.multiple_of(t * tb, tb), tb)
            at = a[rows, :]
            g = mm(at, wg[l, :, cols])
            u = mm(at, wu[l, :, cols])
            dhid = mm(dh[rows, :], wd[l, cols, :], NT).astype(bf16).astype(f32)
            sg = sigmoid(g)
            s = g * sg
            hid[rows, :] = (s * u).astype(bf16)
            S[pl.ds(pl.multiple_of(du0 + t * tb, 16), tb), :] = (dhid * s).astype(bf16)
            S[pl.ds(pl.multiple_of(dg0 + t * tb, 16), tb), :] = (dhid * u * (sg + s * (1.0 - sg))).astype(bf16)
            return q
        q = lax.fori_loop(0, T // tb, tokens, q, unroll=True)
        base = b * BR
        def gate_up(w, k):
            for e in range(2 * n):
                S[pl.ds(pl.multiple_of(base + e * CH + k * H, 16), H), :] = w[e * H:(e + 1) * H]
        def down(w):
            for e in range(2 * n):
                for cg in range(ncg):
                    S[pl.ds(pl.multiple_of(base + e * CH + 2 * H + cg * hr, 16), hr), :] = w[e * hr:(e + 1) * hr, cg * BW:(cg + 1) * BW]
        dgv = lambda: S[pl.ds(pl.multiple_of(dg0, 16), T), :]
        duv = lambda: S[pl.ds(pl.multiple_of(du0, 16), T), :]
        q = ops(q, pace2, b)
        w = mm(aT[...], jnp.concatenate([dgv(), duv()], axis=1)).astype(bf16)
        gate_up(w[:, :BW], 0)
        gate_up(w[:, BW:], 1)
        down(mm(hid[...], dh[...], TN).astype(bf16))
        return q

    for c in last_loads + [dy_load, down_loads[1]]:
        c.wait()
    if comm:
        pl.semaphore_wait(barrier, n - 1)

    def between(q):
        def d_input(t, q):
            q = ops(q, cfg["pace"][2], NB)
            rows = pl.ds(pl.multiple_of(t * tt, tt), tt)
            dg = jnp.concatenate([S[pl.ds(pl.multiple_of(GB + j * 2 * T + t * tt, 16), tt), :] for j in range(NB)], axis=1)
            du = jnp.concatenate([S[pl.ds(pl.multiple_of(GB + j * 2 * T + T + t * tt, 16), tt), :] for j in range(NB)], axis=1)
            da = (mm(dg, wg[1], NT).astype(bf16).astype(f32) + mm(du, wu[1], NT).astype(bf16).astype(f32)).astype(bf16).astype(f32)
            wide = xh[rows, :].astype(f32)
            scale = rms_scale(wide)
            dot = jnp.sum(da * wide, -1, keepdims=True)
            dw = da * scale - wide * (scale * scale * scale * dot * (1.0 / D))
            dh[rows, :] = (dh[rows, :].astype(f32) + dw.astype(bf16).astype(f32)).astype(bf16)
            pltpu.make_async_copy(x_in.at[rows, :], xh.at[rows, :], x_sem).start()
            return q
        q = lax.fori_loop(0, T // tt, d_input, q)
        def renorm(t, q):
            rows = pl.ds(pl.multiple_of(t * tt, tt), tt)
            wide = xh[rows, :].astype(f32)
            a0 = (wide * rms_scale(wide)).astype(bf16)
            a[rows, :] = a0
            aT[:, rows] = a0.T
            return q
        pltpu.make_async_copy(x_in, xh, x_sem).wait()
        q = ops(q, 2, NB)
        lax.fori_loop(0, T // tt, renorm, 0)
        return q

    def blocks(b, q):
        q = lax.cond(b == NB, between, lambda q: q, q)
        last = b < NB
        dg0 = jnp.where(last, GB + b * 2 * T, 2 * GB)
        pace = cfg["pace"]
        return block(jnp.where(last, 1, 0), jnp.where(last, b, b - NB), dg0, dg0 + T, b, q,
                     jnp.where(b <= 2, n, jnp.where(last, pace[0], pace[3])), jnp.where(b <= 2, n, jnp.where(last, pace[1], pace[3])))
    q = lax.fori_loop(0, NBLK, blocks, 0)
    if comm:
        lax.fori_loop(q, (LAST + 2) * n, op, 0)
        copies = [
            pltpu.make_async_remote_copy(
                src_ref=ss, dst_ref=squares.at[me], send_sem=sq_send.at[i], recv_sem=sq_recv.at[me],
                device_id={"dp": p}, device_id_type=pl.DeviceIdType.MESH)
            for i, p in enumerate(peers)]
        for c in copies:
            c.start()
        squares[me] = ss[...]
        for k in range(min(6, NB), NB):
            for d in range(2):
                onward(k, d).start()
        for r in range(LAST - RB + 2, LAST + 1):
            for s in range(n - 1):
                for b in range(NBLK):
                    if r - s == (2 * b if b <= ramp else b + ramp if b < NB else b + ramp + gap):
                        for d in range(2):
                            hop(r, s, d).wait_send()
        for i, p in enumerate(peers):
            pltpu.make_async_remote_copy(
                src_ref=ss, dst_ref=squares.at[p], send_sem=sq_send.at[i], recv_sem=sq_recv.at[p],
                device_id={"dp": p}, device_id_type=pl.DeviceIdType.MESH).wait_recv()
        total = squares[0]
        for i in range(1, n):
            total = total + squares[i]
        total = jnp.sum(jnp.sum(total, axis=0, keepdims=True), axis=1, keepdims=True)
        factor[...] = jnp.broadcast_to(jnp.minimum(1.0, 0.5 * lax.rsqrt(total / float(NBLK * BR * BW) + 1e-30)), factor.shape)
        for c in copies:
            c.wait_send()
        for d in range(2):
            for k in range(NB):
                onward(k, d).wait_recv()
                onward(k, d).wait_send()
        for d in range(2):
            for b in range(NBLK):
                pltpu.make_async_copy(S.at[pl.ds(0, CH), :], (own00, own01, own10, own11)[2 * (b // NB) + d].at[b % NB], own_sem.at[d, b]).wait()
    else:
        cps = [pltpu.make_async_copy(S.at[pl.ds(b * BR + d * CH, CH), :], (own00, own01, own10, own11)[2 * (b // NB) + d].at[b % NB], own_sem.at[d, b]) for d in range(2) for b in range(NBLK)]
        for c in cps: c.start()
        for c in cps: c.wait()


def k1(x, dy, wg, wu, wd, n, tt=512, tb=512, comm=True, cid=0, pace=(4, 5, 4, 6), gap=2, unroll=True):
    T, D = x.shape
    F = wg.shape[2]
    NB = F // BW
    NBLK = 2 * NB
    H = D // (2 * n); CH = 3 * H
    GB = NB * 3 * D
    cfg = dict(n=n, T=T, D=D, F=F, tt=min(tt, T), tb=min(tb, T), comm=comm, pace=pace, gap=gap, unroll=unroll)
    any_ = pl.BlockSpec(memory_space=pl.ANY)
    flops = 18 * 2 * T * D * F
    return pl.pallas_call(
        functools.partial(kernel, cfg),
        out_shape=(jax.ShapeDtypeStruct((NB, CH, BW), bf16),) * 6 + (jax.ShapeDtypeStruct((8, 128), f32),),
        in_specs=[any_] * 5,
        out_specs=(any_,) * 6 + (pl.BlockSpec(memory_space=pltpu.VMEM),),
        scratch_shapes=[
            pltpu.VMEM((max(GB + NB * 2 * T, 2 * GB + 2 * T), BW), bf16),
            pltpu.VMEM((T, D), bf16), pltpu.VMEM((T, D), bf16), pltpu.VMEM((D, T), bf16), pltpu.VMEM((T, D), bf16),
            pltpu.VMEM((T, BW), bf16),
            pltpu.VMEM((2, D, F), bf16), pltpu.VMEM((2, D, F), bf16), pltpu.VMEM((2, F, D), bf16),
            pltpu.VMEM((2, RB * (n - 1), CH, BW), bf16),
            pltpu.SemaphoreType.DMA((6,)), pltpu.SemaphoreType.DMA((2, NB)), pltpu.SemaphoreType.DMA, pltpu.SemaphoreType.DMA((2, NBLK)),
            pltpu.SemaphoreType.DMA((2, RB * (n - 1))), pltpu.SemaphoreType.DMA((2, RB * (n - 1))), pltpu.SemaphoreType.REGULAR((2,)),
            pltpu.SemaphoreType.DMA((2, NB)), pltpu.SemaphoreType.DMA((2, NB)),
            pltpu.VMEM((8, 128), f32), pltpu.VMEM((n, 8, 128), f32), pltpu.SemaphoreType.DMA((n - 1,)), pltpu.SemaphoreType.DMA((n,)),
        ],
        compiler_params=pltpu.CompilerParams(vmem_limit_bytes=67043328, collective_id=cid if comm else None, has_side_effects=True),
        cost_estimate=pl.CostEstimate(flops=flops, bytes_accessed=40 * 10**6, transcendentals=0),
        name="grads")(x, dy, wg, wu, wd)


def adam_math(w, m, v, g):
    m = 0.9 * m + 0.1 * g
    v = 0.95 * v + 0.05 * g * g
    step = m * lax.rsqrt(v + 1e-8) + 0.1 * w
    return (w - 0.02 * step).astype(bf16), m, v


def adam_kernel(n, where, fetch, early, fac_hbm, *refs):
    k = len(where)
    pays, ins = refs[:k], refs[k : k + 9]
    scratch = 11 if fetch else 10
    fac, gbuf, wbuf, wdown, fbuf, fdown, fsem, gsem, isem, osem = refs[-scratch:][:10]
    kept = refs[k + 9 : k + 13] if early else (wbuf, wdown, fbuf, fdown)
    left = refs[-scratch - 4 : -scratch] if fetch else ()
    outs = refs[-scratch - len(left) - 9 : -scratch - len(left)]
    me = lax.axis_index("dp")
    fac_load = pltpu.make_async_copy(fac_hbm, fac, fsem)

    def place(buffers, i, a):
        w, down, f, fd = buffers
        which, kind = a // 3, a % 3
        if which == 0:
            return down.at[i] if kind == 2 else w.at[i, kind]
        return fd.at[i, which - 1] if kind == 2 else f.at[i, which - 1, kind]

    def rows(arrays, piece, a):
        layer, d, hops = piece
        chunk = 2 * lax.rem(me + (n - hops if d == 0 else hops), n) + d
        return arrays[a].at[layer, :, chunk] if a % 3 == 2 else arrays[a].at[layer, chunk]

    new = (wbuf, wdown, fbuf, fdown)
    loads = [[] if early else [pltpu.make_async_copy(rows(ins, p, a), place(new, i, a), isem.at[i, a]) for a in range(9)] for i, p in enumerate(where)]
    pay_loads = [pltpu.make_async_copy(pays[i], gbuf.at[i], gsem.at[i]) for i in range(k)]
    stores = [[pltpu.make_async_copy(place(new, i, a), rows(outs, p, a), osem.at[i, a]) for a in range(9)] for i, p in enumerate(where)]
    fetches = [pltpu.make_async_copy(rows(ins, p, a), place(left, i, a), refs[-1].at[i, a]) for i, p in enumerate(fetch) for a in range(9)]
    for i in range(k):
        pay_loads[i].start()
        for kind in range(3):
            for a in range(kind, 9, 3):
                if not early:
                    loads[i][a].start()
        if i == 0:
            fac_load.start()
    for c in fetches:
        c.start()
    hr = wdown.shape[2]
    fac_load.wait()
    factor = fac[0:1, 0:1]
    for i in range(k):
        pay_loads[i].wait()
        def step(kind, at, g):
            old = [place(kept, i, 3 * which + kind)[at] for which in range(3)]
            for which, value in enumerate(adam_math(old[0].astype(f32), old[1], old[2], g.astype(f32) * factor)):
                place(new, i, 3 * which + kind)[at] = value
        for kind in range(3):
            for a in range(kind, 9, 3):
                if not early:
                    loads[i][a].wait()
            def block(j, _):
                if kind < 2:
                    step(kind, (slice(None), pl.ds(pl.multiple_of(j * BW, BW), BW)), gbuf[i, j, kind])
                else:
                    for cg in range(wdown.shape[3] // BW):
                        step(2, (j, slice(None), slice(cg * BW, (cg + 1) * BW)), gbuf[i, j, 2, cg * hr : (cg + 1) * hr])
                return 0
            lax.fori_loop(0, gbuf.shape[1], block, 0)
            for a in range(kind, 9, 3):
                stores[i][a].start()
    for piece in stores:
        for c in piece:
            c.wait()
    for c in fetches:
        c.wait()


def adam_call(n, factor, pieces, ins, prev, fetch=(), early=()):
    k = len(pieces)
    pays = [g for _, g in pieces]
    hbm, vmem = pl.BlockSpec(memory_space=pltpu.HBM), pl.BlockSpec(memory_space=pltpu.VMEM)
    kept = [] if prev is None else list(prev)
    size = k * pays[0].size
    rows, down = ins[0].shape[2:], (ins[2].shape[1],) + ins[2].shape[3:]
    buffers = lambda k: [((k, 2) + rows, bf16), ((k,) + down, bf16), ((k, 2, 2) + rows, f32), ((k, 2) + down, f32)]
    left = [jax.ShapeDtypeStruct(s, t) for s, t in buffers(len(fetch))] if fetch else []
    out = pl.pallas_call(
        functools.partial(adam_kernel, n, tuple(w for w, _ in pieces), tuple(fetch), bool(early)),
        in_specs=[hbm] * (1 + k + 9) + [vmem] * len(early) + [hbm] * len(kept),
        out_specs=[hbm] * 9 + [vmem] * len(left),
        scratch_shapes=[
            pltpu.VMEM(factor.shape, f32), pltpu.VMEM((k,) + pays[0].shape, bf16)] + [pltpu.VMEM(s, t) for s, t in buffers(k)] + [
            pltpu.SemaphoreType.DMA, pltpu.SemaphoreType.DMA((k,)), pltpu.SemaphoreType.DMA((k, 9)), pltpu.SemaphoreType.DMA((k, 9))]
            + ([pltpu.SemaphoreType.DMA((len(fetch), 9))] if fetch else []),
        out_shape=[jax.ShapeDtypeStruct(x.shape, x.dtype) for x in ins] + left,
        input_output_aliases={} if prev is None else {1 + k + 9 + len(early) + i: i for i in range(9)},
        compiler_params=pltpu.CompilerParams(vmem_limit_bytes=(46 if fetch or early else 62) * 2**20),
        cost_estimate=pl.CostEstimate(flops=10**9 * k, bytes_accessed=22 * size, transcendentals=size),
        name="adamw")(factor, *pays, *ins, *early, *kept)
    return (out[:9], out[9:]) if fetch else out


def views(arrays, n):
    out = []
    for i, a in enumerate(arrays):
        L, r, c = a.shape
        out.append(a.reshape(L, 2 * n, r // (2 * n), c) if i % 3 < 2 else a.reshape(L, r // BW, 2 * n, BW // (2 * n), c))
    return out


def solution(mesh):
    n = mesh.shape["dp"]
    to = ([(i, (i + 1) % n) for i in range(n)], [(i, (i - 1) % n) for i in range(n)])

    def step(x, dy, *arrays):
        *sums, factor = k1(x[0], dy[0], *arrays[:3], n)
        _, _, F = arrays[0].shape
        ins = views(arrays, n)
        last, first, came = ([o.reshape(F // BW, 3, o.shape[1] // 3, BW) for o in sums[i : i + 2]] for i in (0, 2, 4))

        def pieces(layer, pays, hops):
            return [((layer, d, hops), pays[d]) for d in range(2)]

        waiting = pieces(1, last, 0) + pieces(0, first, 0) + pieces(1, came, 1)
        outs, last = None, came
        for s in range(1, n):
            ahead = []
            first = list(first)
            for d in range(2):
                first[d] = lax.ppermute(first[d], "dp", to[d])
            if s < n - 1:
                for d in range(2):
                    ahead.append(lax.ppermute(last[d], "dp", to[d]))
            if s < n - 1:
                outs = adam_call(n, factor, waiting, ins, outs)
            else:
                outs = adam_call(n, factor, waiting[:2], ins, outs)
                outs, early = adam_call(n, factor, waiting[2:], ins, outs, [w for w, _ in pieces(0, first, s)])
            waiting = pieces(0, first, s) + (pieces(1, ahead, s + 1) if ahead else [])
            last = ahead
        outs = adam_call(n, factor, waiting, ins, outs, early=early)
        return tuple(o.reshape(w.shape) for o, w in zip(outs, arrays))

    step = jax.shard_map(
        step,
        mesh=mesh,
        in_specs=(P(("rep", "dp"), None, None),) * 2 + (P(None, None, None),) * 9,
        out_specs=(P("rep", None, None),) * 9,
        check_vma=False,
    )
    return step
```
